256 devices in a mesh: dp: 8 (over y, core), head: 2 (over z_lo), kv: 16 (over z_hi, x).
Axes of the slice: x: 4, y: 4, z: 8 (z_hi: 4, z_lo: 2; z = z_hi * 2 + z_lo), core: 2. Of those that a mesh axis runs over, the one named last changes fastest.
Arguments:
- teacher_query: bfloat16 [8, 4096, 3584], P('dp', 'kv', 'head'), may hold values from -96 to 96
- teacher_key: bfloat16 [8, 4096, 512], P('dp', 'kv', 'head'), may hold values from -8 to 8
- student_query: bfloat16 [8, 4096, 1792], P('dp', 'kv', 'head'), may hold values from -96 to 96
- student_key: bfloat16 [8, 4096, 256], P('dp', 'kv', 'head'), may hold values from -8 to 8
- pair_table: int32 [14, 2], replicated, may hold values from 0 to 27, as said below
Outputs:
- kl: float32 [8, 14, 4096], P('dp', 'head', 'kv')
- head_loss: float32 [14], P('head')
The draws below stay inside these ranges and needn't reach their ends.
Inputs may be any that keep to these rules, and one draw needn't show every extreme that they name: `pair_table`: each of the 28 teacher heads appears exactly once in the table.
All inputs are finite; a program needn't handle non-finite values.
Results may differ from the reference program's by a relative error of at most 0.0003.
Values may be sent and summed in bfloat16 or wider, within the bound.
A program may use at most 64 MiB of HBM per device.

```python
import math
import jax
import jax.numpy as jnp
from jax import lax

HT = 28
KVT = 4
DH = 128
HS = 14
KVS = 2
L = 4096
SEQS = 8


def key_field(key, heads):
    shape = (SEQS, L, heads, DH)
    row_scale = jnp.exp(jax.random.uniform(jax.random.fold_in(key, 1), (SEQS, L, heads, 1), jnp.float32, math.log(0.5), math.log(2.0)))
    base = jnp.clip(jax.random.normal(key, shape, jnp.float32), -4.0, 4.0)
    return base * row_scale


def query_field(key, heads):
    shape = (SEQS, L, heads, DH)
    row_scale = jnp.exp(jax.random.uniform(jax.random.fold_in(key, 1), (SEQS, L, heads, 1), jnp.float32, math.log(0.3), math.log(3.0)))
    return jnp.clip(jax.random.normal(key, shape, jnp.float32), -5.0, 5.0) * row_scale


def draw_teacher_key(key, part):
    keys = key_field(jax.random.fold_in(key, 11), KVT)
    return keys.reshape(SEQS, L, KVT * DH).astype(jnp.bfloat16)


def draw_student_key(key, part):
    keys = key_field(jax.random.fold_in(key, 12), KVS)
    return keys.reshape(SEQS, L, KVS * DH).astype(jnp.bfloat16)


def draw_teacher_query(key, part):
    queries = query_field(jax.random.fold_in(key, 13), HT)
    return queries.reshape(SEQS, L, HT * DH).astype(jnp.bfloat16)


def draw_student_query(key, part):
    queries = query_field(jax.random.fold_in(key, 14), HS)
    return queries.reshape(SEQS, L, HS * DH).astype(jnp.bfloat16)


def draw_pair_table(key, part):
    order = jax.random.permutation(jax.random.fold_in(key, 15), HT)
    return order.astype(jnp.int32).reshape(HS, 2)


def setup_inputs(seed: int = 0) -> dict:
    streams_of = jax.random.split(jax.random.key(seed), 6)
    teacher_query = draw_teacher_query(jax.random.fold_in(streams_of[5], 71), 0)
    teacher_key = draw_teacher_key(jax.random.fold_in(streams_of[5], 71), 0)
    student_query = draw_student_query(jax.random.fold_in(streams_of[5], 71), 0)
    student_key = draw_student_key(jax.random.fold_in(streams_of[5], 71), 0)
    pair_table = draw_pair_table(jax.random.fold_in(streams_of[5], 71), 0)
    return dict(teacher_query=teacher_query, teacher_key=teacher_key, student_query=student_query, student_key=student_key, pair_table=pair_table)


masked_value = -1e+30

def masked_logits(query_rows, key_rows, causal_mask):
    scale = 1.0 / math.sqrt(DH)
    product = jnp.dot(query_rows.astype(jnp.float32), key_rows.astype(jnp.float32).T, precision=lax.Precision.HIGHEST, preferred_element_type=jnp.float32) * scale
    return jnp.where(causal_mask, product, masked_value)

def log_total(logits, causal_mask):
    row_max = lax.optimization_barrier(jnp.max(logits, axis=-1))
    weights = jnp.where(causal_mask, jnp.exp(logits - row_max[:, None]), 0.0)
    return row_max + jnp.log(lax.optimization_barrier(jnp.sum(weights, axis=-1)))

def reference(teacher_query, teacher_key, student_query, student_key, pair_table):
    teacher_q = teacher_query.reshape(SEQS, L, HT, DH)
    teacher_k = teacher_key.reshape(SEQS, L, KVT, DH)
    student_q = student_query.reshape(SEQS, L, HS, DH)
    student_k = student_key.reshape(SEQS, L, KVS, DH)
    group_teacher = HT // KVT
    group_student = HS // KVS
    positions = jnp.arange(L, dtype=jnp.int32)
    causal_mask = positions[None, :] <= positions[:, None]

    def one_item(flat_index):
        sequence = flat_index // HS
        student = flat_index % HS
        s_logits = masked_logits(student_q[sequence, :, student], student_k[sequence, :, student // group_student], causal_mask)
        s_lse = log_total(s_logits, causal_mask)
        total = jnp.zeros((L,), jnp.float32)
        for column in range(2):
            teacher = pair_table[student, column]
            t_logits = masked_logits(teacher_q[sequence, :, teacher], teacher_k[sequence, :, teacher // group_teacher], causal_mask)
            t_lse = log_total(t_logits, causal_mask)
            probs = jnp.where(causal_mask, jnp.exp(t_logits - t_lse[:, None]), 0.0)
            total = total + (lax.optimization_barrier(jnp.sum(probs * (t_logits - s_logits), axis=-1)) - t_lse + s_lse)
        return total
    kl = lax.map(one_item, jnp.arange(SEQS * HS, dtype=jnp.int32)).reshape(SEQS, HS, L)
    head_loss = lax.optimization_barrier(jnp.sum(kl, axis=(0, 2))) / (SEQS * L)
    return (kl, head_loss)
```

```python
import math

import jax
import jax.numpy as jnp
from jax import lax
from jax.experimental import pallas as pl
from jax.experimental.pallas import tpu as pltpu
from jax.sharding import PartitionSpec as P

HT = 28
HS = 14
DH = 128
GROUP = 7
NX = 4
NZ = 4
N_KV = NX * NZ
N_DP = 8
ROWS = 256
CHUNK = 128
HALF = CHUNK // 2
TILE = NX * CHUNK
T_LOCAL = 14
S_LOCAL = 7
SCALE = 1.0 / math.sqrt(DH)
LOG2E = math.log2(math.e)
LN2 = math.log(2.0)
NEG = -1e30
MESH = pl.DeviceIdType.MESH
NT = (((1,), (1,)), ((), ()))


def split_scaled(q):
    scaled = q.astype(jnp.float32) * (SCALE * LOG2E)
    hi = scaled.astype(jnp.bfloat16)
    lo = (scaled - hi.astype(jnp.float32)).astype(jnp.bfloat16)
    return jnp.concatenate([hi, lo], axis=1)


def kernel(
    table,
    tq,
    tk_in,
    sq_in,
    sk_in,
    kl_out,
    loss_out,
    keys,
    sq,
    qy,
    qg,
    qs,
    t_state,
    s_state,
    y_a,
    g_a,
    y_b,
    g_b,
    y_s,
    bias,
    contrib,
    kl_other,
    sums_plane,
    sums_dp,
    group_table,
    student_table,
    local_sem,
    swap_send,
    swap_recv,
    z_send,
    z_recv,
    relay_send,
    x1_send,
    x1_recv,
    x2_send,
    x2_recv,
    kl_sem,
    plane_send,
    plane_recv,
    dp_send,
    dp_recv,
):
    dp = lax.axis_index("dp")
    head = lax.axis_index("head")
    kv = lax.axis_index("kv")
    row = kv // NX
    col = kv % NX
    right = row * NX + (col + 1) % NX
    left = row * NX + (col + NX - 1) % NX

    def device(d, h, k):
        return (d, h, k)

    def remote(src, dst, send_sem, recv_sem, dev):
        return pltpu.make_async_remote_copy(
            src_ref=src,
            dst_ref=dst,
            send_sem=send_sem,
            recv_sem=recv_sem,
            device_id=dev,
            device_id_type=MESH,
        )

    s_lane = pl.multiple_of(256 + head * 128, 128)
    fill_t = pltpu.make_async_copy(tk_in.at[0], keys.at[kv, :, pl.ds(0, 256)], local_sem.at[0])
    fill_s = pltpu.make_async_copy(sk_in.at[0], keys.at[kv, :, pl.ds(s_lane, 128)], local_sem.at[1])
    fill_q = pltpu.make_async_copy(sq_in.at[0], sq.at[head], local_sem.at[2])
    fill_s.start()
    fill_t.start()
    fill_q.start()

    barrier = pltpu.get_barrier_semaphore()

    def greet_plane(i, _):
        peer = (head * N_KV + kv + i) % (2 * N_KV)
        pl.semaphore_signal(
            barrier,
            inc=1,
            device_id=device(dp, peer // N_KV, peer % N_KV),
            device_id_type=MESH,
        )
        return 0

    lax.fori_loop(1, 2 * N_KV, greet_plane, 0)

    def greet_dp(i, _):
        pl.semaphore_signal(
            barrier, inc=1, device_id=device((dp + i) % N_DP, head, kv), device_id_type=MESH
        )
        return 0

    lax.fori_loop(1, N_DP, greet_dp, 0)
    pl.semaphore_wait(barrier, 2 * N_KV - 1 + N_DP - 1)

    partner = device(dp, 1 - head, kv)
    fill_s.wait()
    swap_s = remote(
        keys.at[kv, :, pl.ds(s_lane, 128)],
        keys.at[kv, :, pl.ds(s_lane, 128)],
        swap_send.at[0],
        swap_recv.at[0],
        partner,
    )
    swap_s.start()
    fill_q.wait()
    swap_q = remote(sq.at[head], sq.at[head], swap_send.at[1], swap_recv.at[1], partner)

    bias_col = col * ROWS + lax.broadcasted_iota(jnp.int32, (TILE, ROWS), 1)
    bias_pos = lax.broadcasted_iota(jnp.int32, (TILE, ROWS), 0)
    bias_key = bias_pos + (bias_pos // CHUNK) * (ROWS - CHUNK)
    for c in range(2):
        bias[c] = jnp.where(bias_key + c * CHUNK <= bias_col, 0.0, NEG)

    def columns(h):
        return pl.ds(pl.multiple_of(h * DH, DH), DH)

    fill_t.wait()
    other_lane = pl.multiple_of(384 - head * 128, 128)
    landed_s = remote(
        keys.at[kv, :, pl.ds(other_lane, 128)],
        keys.at[kv, :, pl.ds(other_lane, 128)],
        swap_send.at[0],
        swap_recv.at[0],
        partner,
    )
    landed_s.wait_recv()

    def z_copy(slot_row, c, send_sem, target_row):
        block = keys.at[slot_row * NX + col, pl.ds(c * CHUNK, CHUNK)]
        return remote(
            block, block, send_sem, z_recv.at[slot_row, c], device(dp, head, target_row * NX + col)
        )

    def up(c):
        return z_copy(row, c, z_send.at[0, c], row + 1)

    def down(c):
        return z_copy(row, c, z_send.at[1, c], (row + NZ - 1) % NZ)

    has_up = row < NZ - 1
    has_down = row < 2

    def forward(slot_row, c):
        return z_copy(slot_row, c, relay_send.at[c], jnp.where(row == 0, NZ - 1, row + 1))

    def x1(slot_row, c, side, target):
        block = keys.at[slot_row * NX + col, pl.ds(c * CHUNK, CHUNK)]
        return remote(
            block,
            block,
            x1_send.at[slot_row, c, side],
            x1_recv.at[slot_row, c, side],
            device(dp, head, target),
        )

    def x1_arrival(slot_row, c, side, source_col):
        block = keys.at[slot_row * NX + source_col, pl.ds(c * CHUNK, CHUNK)]
        return remote(
            block,
            block,
            x1_send.at[slot_row, c, side],
            x1_recv.at[slot_row, c, side],
            device(dp, head, right),
        )

    def x2(slot_row, c, side, source_col, target):
        block = keys.at[
            slot_row * NX + source_col, pl.ds(c * CHUNK + side * HALF, HALF)
        ]
        return remote(
            block,
            block,
            x2_send.at[slot_row, c, side],
            x2_recv.at[slot_row, c, side],
            device(dp, head, target),
        )

    left_col = (col + NX - 1) % NX
    right_col = (col + 1) % NX
    far_col = (col + 2) % NX

    def wave(w):
        early = w < 2
        last = row == NZ - 1
        k = w // 2
        r_last = jnp.where(w >= 6, 1, jnp.where(w % 2 == 0, 2, 0))
        c_last = jnp.where(w >= 6, w - 6, (w - 2) // 2)
        r = jnp.where(early, row, jnp.where(last, r_last, row - k))
        c = jnp.where(early, w, jnp.where(last, c_last, w % 2))
        return r, c

    def start_x1(r, c):
        x1(r, c, 0, right).start()
        x1(r, c, 1, left).start()

    def z_event(w):
        r, c = wave(w)
        z_copy(r, c, relay_send.at[c], row).wait_recv()
        start_x1(r, c)

        @pl.when((row == 1) & (r == 0))
        def _():
            forward(0, c).start()

    def x_event(w):
        r, c = wave(w)
        x1_arrival(r, c, 0, left_col).wait_recv()
        x2(r, c, 0, left_col, right).start()
        x1_arrival(r, c, 1, right_col).wait_recv()
        x2(r, c, 1, right_col, left).start()

    def d_event(w):
        r, c = wave(w)
        x2(r, c, 0, far_col, right).wait_recv()
        x2(r, c, 1, far_col, right).wait_recv()

    for c in range(2):
        start_x1(row, c)

        @pl.when(has_up)
        def _():
            up(c).start()

        @pl.when(has_down)
        def _():
            down(c).start()

    swap_q.start()

    def prepare(t, _):
        qy[t] = split_scaled(tq[0, :, columns(t)])
        t_state[t] = jnp.concatenate(
            [jnp.full((8, ROWS), NEG, jnp.float32), jnp.zeros((16, ROWS), jnp.float32)], axis=0
        )
        return 0

    lax.fori_loop(0, T_LOCAL, prepare, 0)

    def prepare_student(t, _):
        qs[t] = split_scaled(sq[head, :, columns(t)])
        s_state[t] = jnp.concatenate(
            [jnp.full((8, ROWS), NEG, jnp.float32), jnp.zeros((8, ROWS), jnp.float32)], axis=0
        )
        return 0

    lax.fori_loop(0, S_LOCAL, prepare_student, 0)

    waves = 2 * (row + 1)
    x_event(0)
    x_event(1)

    @pl.when(row == 0)
    def _():
        for c in range(2):
            z_copy(1, c, relay_send.at[c], row).wait_recv()
            forward(1, c).start()

    @pl.when(row > 0)
    def _():
        z_event(2)
        z_event(3)

    def student_of(t):
        found = jnp.int32(0)
        for e in range(HT):
            found = jnp.where(table[e] == head * T_LOCAL + t, e // 2, found)
        return found

    students = [student_of(t) for t in range(T_LOCAL)]
    for t in range(T_LOCAL):
        student_table[t] = students[t]
        group_table[t] = jnp.where(students[t] >= GROUP, 1, 0)

    remote(sq.at[1 - head], sq.at[1 - head], swap_send.at[1], swap_recv.at[1], partner).wait_recv()

    def prepare_gap(t, _):
        s = student_table[t]
        student_q = sq[0, :, 0:DH]
        for e in range(1, HS):
            candidate = sq[e // GROUP, :, (e % GROUP) * DH : (e % GROUP + 1) * DH]
            student_q = jnp.where(s == e, candidate, student_q)
        qg[t] = jnp.concatenate([tq[0, :, columns(t)], -student_q], axis=1)
        return 0

    lax.fori_loop(0, T_LOCAL, prepare_gap, 0)

    def compute(r, c, masked):
        def tile(lanes):
            return keys[pl.ds(r * NX, NX), pl.ds(c * CHUNK, CHUNK), lanes].reshape(TILE, 128)

        def product(lhs, rhs):
            return lax.dot_general(lhs, rhs, NT, preferred_element_type=jnp.float32)

        def teacher_products(t, group, lane, y_buf, g_buf):
            k = tile(pl.ds(lane, 128))
            ks = jnp.where(group == 0, tile(pl.ds(256, 128)), tile(pl.ds(384, 128)))
            y_buf[...] = product(jnp.concatenate([k, k], axis=1), qy[t])
            g_buf[...] = product(jnp.concatenate([k, ks], axis=1), qg[t])

        def student_products(t):
            k = tile(pl.ds(s_lane, 128))
            y_s[...] = product(jnp.concatenate([k, k], axis=1), qs[t])

        def weights(y_buf, running_max):
            y = y_buf[...]
            if masked:
                y = y + bias[c]
            y = y.reshape(TILE // 8, 8, ROWS)
            new_max = jnp.maximum(running_max, jnp.max(y, axis=0))
            return new_max, jnp.exp2(running_max - new_max), jnp.exp2(y - new_max[None])

        def teacher_update(t, y_buf, g_buf):
            new_max, rescale, p = weights(y_buf, t_state[t, 0:8])
            t_state[t, 0:8] = new_max
            t_state[t, 8:16] = t_state[t, 8:16] * rescale + jnp.sum(p, axis=0)
            t_state[t, 16:24] = t_state[t, 16:24] * rescale + jnp.sum(
                p * g_buf[...].reshape(p.shape), axis=0
            )

        def student_update(t):
            new_max, rescale, p = weights(y_s, s_state[t, 0:8])
            s_state[t, 0:8] = new_max
            s_state[t, 8:16] = s_state[t, 8:16] * rescale + jnp.sum(p, axis=0)

        teacher_products(0, group_table[0], 0, y_a, g_a)

        def step(j, _):
            following = jnp.minimum(j + 1, GROUP - 1)
            teacher_products(GROUP + j, group_table[GROUP + j], 128, y_b, g_b)
            student_products(j)
            teacher_update(j, y_a, g_a)
            teacher_products(following, group_table[following], 0, y_a, g_a)
            teacher_update(GROUP + j, y_b, g_b)
            student_update(j)
            return 0

        lax.fori_loop(0, GROUP, step, 0)

    for w in range(2):

        @pl.when(w + 4 < waves)
        def _():
            z_event(w + 4)

        @pl.when(w + 2 < waves)
        def _():
            x_event(w + 2)

        d_event(w)
        compute(row, w, True)

    def later(w, _):
        @pl.when(w + 4 < waves)
        def _():
            z_event(w + 4)

        @pl.when(w + 2 < waves)
        def _():
            x_event(w + 2)

        d_event(w)
        r, c = wave(w)
        compute(r, c, False)
        return 0

    lax.fori_loop(2, waves, later, 0)

    lane_row = lax.broadcasted_iota(jnp.int32, (8, ROWS), 0)
    parts = [jnp.zeros((8, ROWS), jnp.float32), jnp.zeros((8, ROWS), jnp.float32)]
    for t in range(T_LOCAL):
        m = t_state[t, 0:8]
        top = jnp.max(m, axis=0, keepdims=True)
        w = jnp.exp2(m - top)
        total = jnp.sum(t_state[t, 8:16] * w, axis=0, keepdims=True)
        cross = jnp.sum(t_state[t, 16:24] * w, axis=0, keepdims=True)
        value = cross / total * SCALE - (top + jnp.log2(total)) * LN2
        for g in range(2):
            parts[g] = parts[g] + jnp.where(lane_row == students[t] - g * GROUP, value, 0.0) * jnp.where(
                (students[t] >= GROUP) == (g == 1), 1.0, 0.0
            )
    home = jnp.zeros((8, ROWS), jnp.float32)
    for t in range(S_LOCAL):
        m = s_state[t, 0:8]
        top = jnp.max(m, axis=0, keepdims=True)
        total = jnp.sum(s_state[t, 8:16] * jnp.exp2(m - top), axis=0, keepdims=True)
        home = home + jnp.where(lane_row == t, (top + jnp.log2(total)) * (2.0 * LN2), 0.0)
    for g in range(2):
        contrib[g] = parts[g] + jnp.where(head == g, home, 0.0)
    kl_copy = remote(contrib.at[1 - head], kl_other, kl_sem.at[0], kl_sem.at[1], partner)
    kl_copy.start()

    me = head * N_KV + kv
    for g in range(2):
        block = jnp.sum(contrib[g], axis=1, keepdims=True)
        sums_plane[2 * N_KV + g] = jnp.broadcast_to(block, (8, 128))

    def plane_copy(i):
        peer = (me + i) % (2 * N_KV)
        return remote(
            sums_plane.at[2 * N_KV + peer // N_KV],
            sums_plane.at[me],
            plane_send.at[i],
            plane_recv.at[me],
            device(dp, peer // N_KV, peer % N_KV),
        )

    def plane_start(i, _):
        plane_copy(i).start()
        return 0

    lax.fori_loop(1, 2 * N_KV, plane_start, 0)

    kl_copy.wait()
    kl_out[0] = (contrib[head] + kl_other[...])[0:S_LOCAL]

    def plane_wait(i, total):
        source = (me + i) % (2 * N_KV)
        remote(
            sums_plane.at[source],
            sums_plane.at[source],
            plane_send.at[i],
            plane_recv.at[source],
            partner,
        ).wait_recv()
        return total + sums_plane[source]

    plane_total = lax.fori_loop(1, 2 * N_KV, plane_wait, sums_plane[2 * N_KV + head])
    sums_dp[N_DP] = plane_total

    def dp_copy(i):
        return remote(
            sums_dp.at[N_DP],
            sums_dp.at[dp],
            dp_send.at[i],
            dp_recv.at[dp],
            device((dp + i) % N_DP, head, kv),
        )

    for i in range(1, N_DP):
        dp_copy(i).start()
    grand = plane_total
    for i in range(1, N_DP):
        source = (dp + i) % N_DP
        remote(
            sums_dp.at[source], sums_dp.at[source], dp_send.at[i], dp_recv.at[source], partner
        ).wait_recv()
        grand = grand + sums_dp[source]
    loss_out[...] = grand * (1.0 / (N_DP * N_KV * ROWS))

    swap_s.wait_send()
    swap_q.wait_send()
    for c in range(2):

        @pl.when(has_up)
        def _():
            up(c).wait_send()

        @pl.when(has_down)
        def _():
            down(c).wait_send()

        @pl.when(row == 0)
        def _():
            forward(1, c).wait_send()

        @pl.when(row == 1)
        def _():
            forward(0, c).wait_send()

    def drain(w, _):
        r, c = wave(w)
        x1(r, c, 0, right).wait_send()
        x1(r, c, 1, left).wait_send()
        x2(r, c, 0, left_col, right).wait_send()
        x2(r, c, 1, right_col, left).wait_send()
        return 0

    lax.fori_loop(0, waves, drain, 0)

    def plane_drain(i, _):
        plane_copy(i).wait_send()
        return 0

    lax.fori_loop(1, 2 * N_KV, plane_drain, 0)
    for i in range(1, N_DP):
        dp_copy(i).wait_send()


def per_device(teacher_query, teacher_key, student_query, student_key, pair_table):
    vmem = pl.BlockSpec(memory_space=pltpu.VMEM)
    anywhere = pl.BlockSpec(memory_space=pl.ANY)
    dma = pltpu.SemaphoreType.DMA
    f32, bf16 = jnp.float32, jnp.bfloat16
    kl, loss = pl.pallas_call(
        kernel,
        out_shape=(
            jax.ShapeDtypeStruct((1, S_LOCAL, ROWS), f32),
            jax.ShapeDtypeStruct((8, 128), f32),
        ),
        in_specs=[pl.BlockSpec(memory_space=pltpu.SMEM), vmem, anywhere, anywhere, anywhere],
        out_specs=(vmem, vmem),
        scratch_shapes=[
            pltpu.VMEM((N_KV, ROWS, 512), bf16),
            pltpu.VMEM((2, ROWS, S_LOCAL * DH), bf16),
            pltpu.VMEM((T_LOCAL, ROWS, 256), bf16),
            pltpu.VMEM((T_LOCAL, ROWS, 256), bf16),
            pltpu.VMEM((S_LOCAL, ROWS, 256), bf16),
            pltpu.VMEM((T_LOCAL, 24, ROWS), f32),
            pltpu.VMEM((S_LOCAL, 16, ROWS), f32),
            pltpu.VMEM((TILE, ROWS), f32),
            pltpu.VMEM((TILE, ROWS), f32),
            pltpu.VMEM((TILE, ROWS), f32),
            pltpu.VMEM((TILE, ROWS), f32),
            pltpu.VMEM((TILE, ROWS), f32),
            pltpu.VMEM((2, TILE, ROWS), f32),
            pltpu.VMEM((2, 8, ROWS), f32),
            pltpu.VMEM((8, ROWS), f32),
            pltpu.VMEM((2 * N_KV + 2, 8, 128), f32),
            pltpu.VMEM((N_DP + 1, 8, 128), f32),
            pltpu.SMEM((T_LOCAL,), jnp.int32),
            pltpu.SMEM((T_LOCAL,), jnp.int32),
            dma((3,)),
            dma((2,)),
            dma((2,)),
            dma((2, 2)),
            dma((NZ, 2)),
            dma((2,)),
            dma((NZ, 2, 2)),
            dma((NZ, 2, 2)),
            dma((NZ, 2, 2)),
            dma((NZ, 2, 2)),
            dma((2,)),
            dma((2 * N_KV,)),
            dma((2 * N_KV,)),
            dma((N_DP,)),
            dma((N_DP,)),
        ],
        compiler_params=pltpu.CompilerParams(
            collective_id=0, has_side_effects=True, vmem_limit_bytes=60 * 1024 * 1024
        ),
    )(pair_table.reshape(-1), teacher_query, teacher_key, student_query, student_key)
    return kl, loss[:S_LOCAL, 0]


def solution(mesh):
    spec = P("dp", "kv", "head")
    return jax.shard_map(
        per_device,
        mesh=mesh,
        in_specs=(spec, spec, spec, spec, P()),
        out_specs=(P("dp", "head", "kv"), P("head")),
        check_vma=False,
    )
```

```python
import functools
import math

import jax
import jax.numpy as jnp
from jax import lax
from jax.experimental import pallas as pl
from jax.experimental.pallas import tpu as pltpu
from jax.sharding import PartitionSpec as P

HT = 28
HS = 14
DH = 128
GROUP = 7
NX = 4
NZ = 4
N_KV = NX * NZ
N_DP = 8
ROWS = 256
CHUNK = 128
HALF = CHUNK // 2
PIECE = NX * CHUNK
TILE = 2 * PIECE
SUB = 128
T_LOCAL = 14
S_LOCAL = 7
SCALE = 1.0 / math.sqrt(DH)
LOG2E = math.log2(math.e)
LN2 = math.log(2.0)
NEG = -1e30
MESH = pl.DeviceIdType.MESH
NT = (((1,), (1,)), ((), ()))


def split_scaled(q):
    scaled = q.astype(jnp.float32) * (SCALE * LOG2E)
    hi = scaled.astype(jnp.bfloat16)
    lo = (scaled - hi.astype(jnp.float32)).astype(jnp.bfloat16)
    return jnp.concatenate([hi, lo], axis=1)


def kernel(
    table,
    tq,
    tk_in,
    sq_in,
    sk_in,
    kl_out,
    loss_out,
    keys,
    sq,
    qy,
    qg,
    qs,
    t_state,
    s_state,
    y_a,
    g_a,
    y_b,
    g_b,
    y_s,
    bias,
    contrib,
    kl_other,
    sums_plane,
    sums_dp,
    group_table,
    student_table,
    levels,
    local_sem,
    swap_send,
    swap_recv,
    z_send,
    z_recv,
    relay_send,
    x1_send,
    x1_recv,
    x2_send,
    x2_recv,
    kl_sem,
    plane_send,
    plane_recv,
    dp_send,
    dp_recv,
):
    dp = lax.axis_index("dp")
    head = lax.axis_index("head")
    kv = lax.axis_index("kv")
    row = kv // NX
    col = kv % NX
    right = row * NX + (col + 1) % NX
    left = row * NX + (col + NX - 1) % NX

    def device(d, h, k):
        return (d, h, k)

    def remote(src, dst, send_sem, recv_sem, dev):
        return pltpu.make_async_remote_copy(
            src_ref=src,
            dst_ref=dst,
            send_sem=send_sem,
            recv_sem=recv_sem,
            device_id=dev,
            device_id_type=MESH,
        )

    s_lane = pl.multiple_of(256 + head * 128, 128)
    fill_t = pltpu.make_async_copy(tk_in.at[0], keys.at[kv, :, pl.ds(0, 256)], local_sem.at[0])
    fill_s = pltpu.make_async_copy(sk_in.at[0], keys.at[kv, :, pl.ds(s_lane, 128)], local_sem.at[1])
    fill_q = pltpu.make_async_copy(sq_in.at[0], sq.at[head], local_sem.at[2])
    fill_s.start()
    fill_t.start()
    fill_q.start()

    partner = device(dp, 1 - head, kv)
    near = (
        partner,
        device(dp, head, right),
        device(dp, head, left),
        device(dp, head, (kv + NX) % N_KV),
        device(dp, head, (kv + N_KV - NX) % N_KV),
    )
    barrier = pltpu.get_barrier_semaphore()

    def greet_near(semaphore):
        for peer in near:
            pl.semaphore_signal(semaphore, inc=1, device_id=peer, device_id_type=MESH)

    greet_near(barrier)
    for i in range(1, N_DP):
        pl.semaphore_signal(
            barrier, inc=1, device_id=device((dp + i) % N_DP, head, kv), device_id_type=MESH
        )

    def columns(h):
        return pl.ds(pl.multiple_of(h * DH, DH), DH)

    fill_q.wait()

    def prepare_student(t, _):
        qs[t] = split_scaled(sq[head, :, columns(t)])
        s_state[t] = jnp.concatenate(
            [jnp.full((8, ROWS), NEG, jnp.float32), jnp.zeros((8, ROWS), jnp.float32)], axis=0
        )
        return 0

    lax.fori_loop(0, S_LOCAL, prepare_student, 0)
    bias_col = col * ROWS + lax.broadcasted_iota(jnp.int32, (PIECE, ROWS), 1)
    bias_pos = lax.broadcasted_iota(jnp.int32, (PIECE, ROWS), 0)
    bias_key = bias_pos + (bias_pos // CHUNK) * (ROWS - CHUNK)
    for c in range(2):
        bias[c * PIECE : (c + 1) * PIECE] = jnp.where(bias_key + c * CHUNK <= bias_col, 0.0, NEG)
    fill_s.wait()
    fill_t.wait()
    pl.semaphore_wait(barrier, len(near) + N_DP - 1)

    swap_s = remote(
        keys.at[kv, :, pl.ds(s_lane, 128)],
        keys.at[kv, :, pl.ds(s_lane, 128)],
        swap_send.at[0],
        swap_recv.at[0],
        partner,
    )
    swap_s.start()
    greet_near(levels.at[0])
    swap_q = remote(sq.at[head], sq.at[head], swap_send.at[1], swap_recv.at[1], partner)
    last_row = row == NZ - 1

    @pl.when(last_row)
    def _():
        swap_q.start()


    def student_of(t):
        found = jnp.int32(0)
        for e in range(HT):
            found = jnp.where(table[e // 2, e % 2] == head * T_LOCAL + t, e // 2, found)
        return found

    students = [student_of(t) for t in range(T_LOCAL)]
    for t in range(T_LOCAL):
        student_table[t] = students[t]
        group_table[t] = jnp.where(students[t] >= GROUP, 1, 0)

    def prepare(t, _):
        q = tq[0, :, columns(t)]
        qy[t] = split_scaled(q)
        s = student_table[t]
        minus_q = jnp.zeros((ROWS, DH), jnp.bfloat16)
        for e in range(S_LOCAL):
            candidate = -sq[head, :, e * DH : (e + 1) * DH]
            minus_q = jnp.where(s == head * S_LOCAL + e, candidate, minus_q)
        qg[t] = jnp.concatenate([q, minus_q], axis=1)
        t_state[t] = jnp.concatenate(
            [jnp.full((8, ROWS), NEG, jnp.float32), jnp.zeros((16, ROWS), jnp.float32)], axis=0
        )
        return 0

    lax.fori_loop(0, T_LOCAL, prepare, 0)
    other_lane = pl.multiple_of(384 - head * 128, 128)
    landed_s = remote(
        keys.at[kv, :, pl.ds(other_lane, 128)],
        keys.at[kv, :, pl.ds(other_lane, 128)],
        swap_send.at[0],
        swap_recv.at[0],
        partner,
    )
    landed_s.wait_recv()

    def z_copy(slot_row, c, send_sem, target_row):
        block = keys.at[slot_row * NX + col, pl.ds(c * CHUNK, CHUNK)]
        return remote(
            block, block, send_sem, z_recv.at[slot_row, c], device(dp, head, target_row * NX + col)
        )

    def up(c):
        return z_copy(row, c, z_send.at[0, c], row + 1)

    def down(c):
        return z_copy(row, c, z_send.at[1, c], (row + NZ - 1) % NZ)

    has_up = row < NZ - 1
    has_down = (row == 0, row < 2)

    def forward(slot_row, c):
        return z_copy(slot_row, c, relay_send.at[c], jnp.where(row == 0, NZ - 1, jnp.where(row == NZ - 1, 2, row + 1)))

    def x1(slot_row, c, side, target):
        block = keys.at[slot_row * NX + col, pl.ds(c * CHUNK, CHUNK)]
        return remote(
            block,
            block,
            x1_send.at[slot_row, c, side],
            x1_recv.at[slot_row, c, side],
            device(dp, head, target),
        )

    def x1_arrival(slot_row, c, side, source_col):
        block = keys.at[slot_row * NX + source_col, pl.ds(c * CHUNK, CHUNK)]
        return remote(
            block,
            block,
            x1_send.at[slot_row, c, side],
            x1_recv.at[slot_row, c, side],
            device(dp, head, right),
        )

    def x2(slot_row, c, side, source_col, target):
        block = keys.at[
            slot_row * NX + source_col, pl.ds(c * CHUNK + side * HALF, HALF)
        ]
        return remote(
            block,
            block,
            x2_send.at[slot_row, c, side],
            x2_recv.at[slot_row, c, side],
            device(dp, head, target),
        )

    left_col = (col + NX - 1) % NX
    right_col = (col + 1) % NX
    far_col = (col + 2) % NX

    def wave(w):
        early = w < 2
        last = row == NZ - 1
        k = w // 2
        r_last = jnp.where(w >= 6, 1, jnp.where(w % 2 == 0, 2, 0))
        c_last = jnp.where(w >= 6, w - 6, (w - 2) // 2)
        r = jnp.where(early, row, jnp.where(last, r_last, row - k))
        c = jnp.where(early, w, jnp.where(last, c_last, w % 2))
        return r, c

    def start_x1(r, c):
        x1(r, c, 0, right).start()
        x1(r, c, 1, left).start()

    def z_event(w):
        r, c = wave(w)
        z_copy(r, c, relay_send.at[c], row).wait_recv()
        start_x1(r, c)

        @pl.when(((row == NZ - 1) & (r == 0)) | ((row == 2) & (r == 1) & (c == 0)))
        def _():
            forward(r, c).start()

    def x_event(w):
        r, c = wave(w)
        x1_arrival(r, c, 0, left_col).wait_recv()
        x2(r, c, 0, left_col, right).start()
        x1_arrival(r, c, 1, right_col).wait_recv()
        x2(r, c, 1, right_col, left).start()

    def d_event(w):
        r, c = wave(w)
        x2(r, c, 0, far_col, right).wait_recv()
        x2(r, c, 1, far_col, right).wait_recv()

    def start_z(c):
        @pl.when(has_up)
        def _():
            up(c).start()

        @pl.when(has_down[c])
        def _():
            down(c).start()

    for c in range(2):
        start_x1(row, c)
    start_z(0)

    @pl.when(jnp.logical_not(last_row))
    def _():
        swap_q.start()

    waves = 2 * (row + 1)

    def events(event, *indices):
        for w in indices:

            @pl.when(w < waves)
            def _():
                event(w)

    def next_level(i):
        pl.semaphore_wait(levels.at[i - 1], len(near))
        greet_near(levels.at[i])

    x_event(0)
    x_event(1)
    start_z(1)
    next_level(1)

    @pl.when(last_row)
    def _():
        events(z_event, 2, 3)

    remote(sq.at[1 - head], sq.at[1 - head], swap_send.at[1], swap_recv.at[1], partner).wait_recv()

    @pl.when(row == 0)
    def _():
        z_copy(1, 1, relay_send.at[1], row).wait_recv()
        forward(1, 1).start()

    def prepare_far(t, _):
        s = student_table[t]
        minus_q = qg[t, :, DH : 2 * DH]
        for e in range(S_LOCAL):
            candidate = -sq[1 - head, :, e * DH : (e + 1) * DH]
            minus_q = jnp.where(s == (1 - head) * S_LOCAL + e, candidate, minus_q)
        qg[t, :, DH : 2 * DH] = minus_q
        return 0

    lax.fori_loop(0, T_LOCAL, prepare_far, 0)

    def pieces_of(k):
        return wave(2 * k), wave(2 * k + 1)

    def tile(pieces, lane):
        return jnp.concatenate(
            [
                keys[pl.ds(r * NX, NX), pl.ds(c * CHUNK, CHUNK), pl.ds(lane, 128)].reshape(
                    PIECE, 128
                )
                for r, c in pieces
            ],
            axis=0,
        )

    def product(lhs, rhs):
        return lax.dot_general(lhs, rhs, NT, preferred_element_type=jnp.float32)

    def teacher_products(pieces, t, lane, y_buf, g_buf):
        group = group_table[t]
        k_t = tile(pieces, lane)
        k_s = jnp.where(group == 0, tile(pieces, 256), tile(pieces, 384))
        y_buf[...] = product(jnp.concatenate([k_t, k_t], axis=1), qy[t])
        g_buf[...] = product(jnp.concatenate([k_t, k_s], axis=1), qg[t])

    def student_products(pieces, t):
        k_s = tile(pieces, s_lane)
        y_s[...] = product(jnp.concatenate([k_s, k_s], axis=1), qs[t])

    def weights(y_buf, part, running_max, masked):
        y = y_buf[part]
        if masked:
            y = y + bias[part]
        y = y.reshape(SUB // 8, 8, ROWS)
        new_max = jnp.maximum(running_max, jnp.max(y, axis=0))
        return new_max, jnp.exp2(running_max - new_max), jnp.exp2(y - new_max[None])

    parts_of_tile = [pl.ds(n * SUB, SUB) for n in range(TILE // SUB)]

    def teacher_update(t, y_buf, g_buf, masked):
        m, total, cross = t_state[t, 0:8], t_state[t, 8:16], t_state[t, 16:24]
        for part in parts_of_tile:
            m, rescale, p = weights(y_buf, part, m, masked)
            total = total * rescale + jnp.sum(p, axis=0)
            cross = cross * rescale + jnp.sum(p * g_buf[part].reshape(p.shape), axis=0)
        t_state[t, 0:8] = m
        t_state[t, 8:16] = total
        t_state[t, 16:24] = cross

    def student_update(t, masked):
        m, total = s_state[t, 0:8], s_state[t, 8:16]
        for part in parts_of_tile:
            m, rescale, p = weights(y_s, part, m, masked)
            total = total * rescale + jnp.sum(p, axis=0)
        s_state[t, 0:8] = m
        s_state[t, 8:16] = total

    def step(masked, now, after, j, _):
        final = j == GROUP - 1
        later = [
            tuple(jnp.where(final, new, old) for old, new in zip(*pair)) for pair in zip(now, after)
        ]
        teacher_products(now, GROUP + j, 128, y_b, g_b)
        student_products(now, j)
        teacher_update(j, y_a, g_a, masked)
        teacher_products(later, jnp.where(final, 0, j + 1), 0, y_a, g_a)
        teacher_update(GROUP + j, y_b, g_b, masked)
        student_update(j, masked)
        return 0

    d_event(0)
    d_event(1)
    teacher_products(pieces_of(0), 0, 0, y_a, g_a)

    def stretch(masked, n, _):
        k = n // 3
        part = n % 3

        if masked:

            @pl.when((part == 1) & last_row)
            def _():
                events(x_event, 2, 3)
                events(z_event, 4, 5)

            @pl.when((part == 1) & jnp.logical_not(last_row))
            def _():
                events(z_event, 2, 3)

            @pl.when((part == 2) & jnp.logical_not(last_row))
            def _():
                events(x_event, 2, 3)
                events(z_event, 4, 5)

        else:

            @pl.when(part == 0)
            def _():
                events(x_event, 2 * k + 2, 2 * k + 3)
                events(z_event, 2 * k + 4, 2 * k + 5)

        @pl.when(part == 2)
        def _():
            events(d_event, 2 * k + 2, 2 * k + 3)

        lax.fori_loop(
            3 * part,
            jnp.minimum(3 * part + 3, GROUP),
            functools.partial(step, masked, pieces_of(k), pieces_of(jnp.minimum(k + 1, row))),
            0,
        )
        return 0

    lax.fori_loop(0, 3, functools.partial(stretch, True), 0)
    next_level(2)
    lax.fori_loop(3, 3 * (row + 1), functools.partial(stretch, False), 0)

    next_level(3)
    lane_row = lax.broadcasted_iota(jnp.int32, (8, ROWS), 0)
    parts = [jnp.zeros((8, ROWS), jnp.float32), jnp.zeros((8, ROWS), jnp.float32)]
    for t in range(T_LOCAL):
        m = t_state[t, 0:8]
        top = jnp.max(m, axis=0, keepdims=True)
        w = jnp.exp2(m - top)
        total = jnp.sum(t_state[t, 8:16] * w, axis=0, keepdims=True)
        cross = jnp.sum(t_state[t, 16:24] * w, axis=0, keepdims=True)
        value = cross / total * SCALE - (top + jnp.log2(total)) * LN2
        for g in range(2):
            parts[g] = parts[g] + jnp.where(lane_row == students[t] - g * GROUP, value, 0.0) * jnp.where(
                (students[t] >= GROUP) == (g == 1), 1.0, 0.0
            )
    home = jnp.zeros((8, ROWS), jnp.float32)
    for t in range(S_LOCAL):
        m = s_state[t, 0:8]
        top = jnp.max(m, axis=0, keepdims=True)
        total = jnp.sum(s_state[t, 8:16] * jnp.exp2(m - top), axis=0, keepdims=True)
        home = home + jnp.where(lane_row == t, (top + jnp.log2(total)) * (2.0 * LN2), 0.0)
    for g in range(2):
        contrib[g] = parts[g] + jnp.where(head == g, home, 0.0)
    pl.semaphore_wait(levels.at[3], len(near))
    kl_copy = remote(contrib.at[1 - head], kl_other, kl_sem.at[0], kl_sem.at[1], partner)
    kl_copy.start()

    me = head * N_KV + kv
    for g in range(2):
        block = jnp.sum(contrib[g], axis=1, keepdims=True)
        sums_plane[2 * N_KV + g] = jnp.broadcast_to(block, (8, 128))

    def plane_copy(i):
        peer = (me + i) % (2 * N_KV)
        return remote(
            sums_plane.at[2 * N_KV + peer // N_KV],
            sums_plane.at[me],
            plane_send.at[i],
            plane_recv.at[me],
            device(dp, peer // N_KV, peer % N_KV),
        )

    def plane_start(i, _):
        plane_copy(i).start()
        return 0

    lax.fori_loop(1, 2 * N_KV, plane_start, 0)

    kl_copy.wait()
    kl_out[0] = (contrib[head] + kl_other[...])[0:S_LOCAL]

    def plane_wait(i, total):
        source = (me + i) % (2 * N_KV)
        remote(
            sums_plane.at[source],
            sums_plane.at[source],
            plane_send.at[i],
            plane_recv.at[source],
            partner,
        ).wait_recv()
        return total + sums_plane[source]

    plane_total = lax.fori_loop(1, 2 * N_KV, plane_wait, sums_plane[2 * N_KV + head])
    sums_dp[N_DP] = plane_total

    def dp_copy(i):
        return remote(
            sums_dp.at[N_DP],
            sums_dp.at[dp],
            dp_send.at[i],
            dp_recv.at[dp],
            device((dp + i) % N_DP, head, kv),
        )

    for i in range(1, N_DP):
        dp_copy(i).start()
    grand = plane_total
    for i in range(1, N_DP):
        source = (dp + i) % N_DP
        remote(
            sums_dp.at[source], sums_dp.at[source], dp_send.at[i], dp_recv.at[source], partner
        ).wait_recv()
        grand = grand + sums_dp[source]
    loss_out[...] = grand * (1.0 / (N_DP * N_KV * ROWS))

    swap_s.wait_send()
    swap_q.wait_send()
    for c in range(2):

        @pl.when(has_up)
        def _():
            up(c).wait_send()

        @pl.when(has_down[c])
        def _():
            down(c).wait_send()

        @pl.when(row == NZ - 1)
        def _():
            forward(0, c).wait_send()

    @pl.when(row == 0)
    def _():
        forward(1, 1).wait_send()

    @pl.when(row == 2)
    def _():
        forward(1, 0).wait_send()

    def drain(w, _):
        r, c = wave(w)
        x1(r, c, 0, right).wait_send()
        x1(r, c, 1, left).wait_send()
        x2(r, c, 0, left_col, right).wait_send()
        x2(r, c, 1, right_col, left).wait_send()
        return 0

    lax.fori_loop(0, waves, drain, 0)

    def plane_drain(i, _):
        plane_copy(i).wait_send()
        return 0

    lax.fori_loop(1, 2 * N_KV, plane_drain, 0)
    for i in range(1, N_DP):
        dp_copy(i).wait_send()


def per_device(teacher_query, teacher_key, student_query, student_key, pair_table):
    vmem = pl.BlockSpec(memory_space=pltpu.VMEM)
    anywhere = pl.BlockSpec(memory_space=pl.ANY)
    dma = pltpu.SemaphoreType.DMA
    f32, bf16 = jnp.float32, jnp.bfloat16
    kl, loss = pl.pallas_call(
        kernel,
        out_shape=(
            jax.ShapeDtypeStruct((1, S_LOCAL, ROWS), f32),
            jax.ShapeDtypeStruct((8, 128), f32),
        ),
        in_specs=[pl.BlockSpec(memory_space=pltpu.SMEM), vmem, anywhere, anywhere, anywhere],
        out_specs=(vmem, vmem),
        scratch_shapes=[
            pltpu.VMEM((N_KV, ROWS, 512), bf16),
            pltpu.VMEM((2, ROWS, S_LOCAL * DH), bf16),
            pltpu.VMEM((T_LOCAL, ROWS, 256), bf16),
            pltpu.VMEM((T_LOCAL, ROWS, 256), bf16),
            pltpu.VMEM((S_LOCAL, ROWS, 256), bf16),
            pltpu.VMEM((T_LOCAL, 24, ROWS), f32),
            pltpu.VMEM((S_LOCAL, 16, ROWS), f32),
            pltpu.VMEM((TILE, ROWS), f32),
            pltpu.VMEM((TILE, ROWS), f32),
            pltpu.VMEM((TILE, ROWS), f32),
            pltpu.VMEM((TILE, ROWS), f32),
            pltpu.VMEM((TILE, ROWS), f32),
            pltpu.VMEM((TILE, ROWS), f32),
            pltpu.VMEM((2, 8, ROWS), f32),
            pltpu.VMEM((8, ROWS), f32),
            pltpu.VMEM((2 * N_KV + 2, 8, 128), f32),
            pltpu.VMEM((N_DP + 1, 8, 128), f32),
            pltpu.SMEM((T_LOCAL,), jnp.int32),
            pltpu.SMEM((T_LOCAL,), jnp.int32),
            pltpu.SemaphoreType.REGULAR((4,)),
            dma((3,)),
            dma((2,)),
            dma((2,)),
            dma((2, 2)),
            dma((NZ, 2)),
            dma((2,)),
            dma((NZ, 2, 2)),
            dma((NZ, 2, 2)),
            dma((NZ, 2, 2)),
            dma((NZ, 2, 2)),
            dma((2,)),
            dma((2 * N_KV,)),
            dma((2 * N_KV,)),
            dma((N_DP,)),
            dma((N_DP,)),
        ],
        compiler_params=pltpu.CompilerParams(
            collective_id=0, has_side_effects=True, vmem_limit_bytes=60 * 1024 * 1024
        ),
    )(pair_table, teacher_query, teacher_key, student_query, student_key)
    return kl, loss[:S_LOCAL, 0]


def solution(mesh):
    spec = P("dp", "kv", "head")
    return jax.shard_map(
        per_device,
        mesh=mesh,
        in_specs=(spec, spec, spec, spec, P()),
        out_specs=(P("dp", "head", "kv"), P("head")),
        check_vma=False,
    )
```

```python
import functools
import math

import jax
import jax.numpy as jnp
from jax import lax
from jax.experimental import pallas as pl
from jax.experimental.pallas import tpu as pltpu
from jax.sharding import PartitionSpec as P

HT = 28
HS = 14
DH = 128
GROUP = 7
NX = 4
NZ = 4
N_KV = NX * NZ
N_DP = 8
ROWS = 256
CHUNK = 128
HALF = CHUNK // 2
PIECE = NX * CHUNK
TILE = 2 * PIECE
SUB = 128
T_LOCAL = 14
S_LOCAL = 7
SCALE = 1.0 / math.sqrt(DH)
LOG2E = math.log2(math.e)
LN2 = math.log(2.0)
NEG = -1e30
MESH = pl.DeviceIdType.MESH
NT = (((1,), (1,)), ((), ()))


def split_scaled(q):
    scaled = q.astype(jnp.float32) * (SCALE * LOG2E)
    hi = scaled.astype(jnp.bfloat16)
    lo = (scaled - hi.astype(jnp.float32)).astype(jnp.bfloat16)
    return jnp.concatenate([hi, lo], axis=1)


def kernel(
    table,
    tq,
    tk_in,
    sq_in,
    sk_in,
    kl_out,
    loss_out,
    keys,
    sq,
    qy,
    qg,
    qs,
    t_state,
    s_state,
    y_a,
    g_a,
    y_b,
    g_b,
    y_s,
    first_p,
    bias,
    contrib,
    kl_other,
    sums_plane,
    sums_dp,
    group_table,
    student_table,
    levels,
    local_sem,
    swap_send,
    swap_recv,
    z_send,
    z_recv,
    relay_send,
    x1_send,
    x1_recv,
    x2_send,
    x2_recv,
    own_send,
    own_recv,
    kl_sem,
    plane_send,
    plane_recv,
    dp_send,
    dp_recv,
):
    dp = lax.axis_index("dp")
    head = lax.axis_index("head")
    kv = lax.axis_index("kv")
    row = kv // NX
    col = kv % NX
    right = row * NX + (col + 1) % NX
    left = row * NX + (col + NX - 1) % NX

    def device(d, h, k):
        return (d, h, k)

    def remote(src, dst, send_sem, recv_sem, dev):
        return pltpu.make_async_remote_copy(
            src_ref=src,
            dst_ref=dst,
            send_sem=send_sem,
            recv_sem=recv_sem,
            device_id=dev,
            device_id_type=MESH,
        )

    s_lane = pl.multiple_of(256 + head * 128, 128)
    fill_t = pltpu.make_async_copy(tk_in.at[0], keys.at[kv, :, pl.ds(0, 256)], local_sem.at[0])
    fill_s = pltpu.make_async_copy(sk_in.at[0], keys.at[kv, :, pl.ds(s_lane, 128)], local_sem.at[1])
    fill_q = pltpu.make_async_copy(sq_in.at[0], sq.at[head], local_sem.at[2])
    fill_s.start()
    fill_t.start()
    fill_q.start()

    partner = device(dp, 1 - head, kv)
    near = (
        partner,
        device(dp, head, right),
        device(dp, head, left),
        device(dp, head, (kv + NX) % N_KV),
        device(dp, head, (kv + N_KV - NX) % N_KV),
    )
    barrier = pltpu.get_barrier_semaphore()

    def greet_near(semaphore):
        for peer in near:
            pl.semaphore_signal(semaphore, inc=1, device_id=peer, device_id_type=MESH)

    greet_near(barrier)
    for i in range(1, N_DP):
        pl.semaphore_signal(
            barrier, inc=1, device_id=device((dp + i) % N_DP, head, kv), device_id_type=MESH
        )

    def columns(h):
        return pl.ds(pl.multiple_of(h * DH, DH), DH)

    fill_q.wait()

    def prepare_student(t, _):
        qs[t] = split_scaled(sq[head, :, columns(t)])
        return 0

    lax.fori_loop(0, S_LOCAL, prepare_student, 0)
    bias_col = col * ROWS + lax.broadcasted_iota(jnp.int32, (PIECE, ROWS), 1)
    bias_pos = lax.broadcasted_iota(jnp.int32, (PIECE, ROWS), 0)
    bias_key = bias_pos + (bias_pos // CHUNK) * (ROWS - CHUNK)
    for c in range(2):
        bias[c * PIECE : (c + 1) * PIECE] = jnp.where(bias_key + c * CHUNK <= bias_col, 0.0, NEG)
    fill_s.wait()
    fill_t.wait()
    pl.semaphore_wait(barrier, len(near) + N_DP - 1)

    def own_part(c, side, part, target):
        block = keys.at[kv, pl.ds(c * CHUNK, CHUNK), pl.ds(256 * part, 256)]
        return remote(
            block, block, own_send.at[c, side, part], own_recv.at[c, side, part], device(dp, head, target)
        )

    def start_own(part):
        for c in range(2):
            own_part(c, 0, part, right).start()
            own_part(c, 1, part, left).start()

    swap_s = remote(
        keys.at[kv, :, pl.ds(s_lane, 128)],
        keys.at[kv, :, pl.ds(s_lane, 128)],
        swap_send.at[0],
        swap_recv.at[0],
        partner,
    )
    swap_s.start()
    start_own(0)
    greet_near(levels.at[0])
    swap_q = remote(sq.at[head], sq.at[head], swap_send.at[1], swap_recv.at[1], partner)
    last_row = row == NZ - 1

    @pl.when(last_row)
    def _():
        swap_q.start()


    def student_of(t):
        found = jnp.int32(0)
        for e in range(HT):
            found = jnp.where(table[e // 2, e % 2] == head * T_LOCAL + t, e // 2, found)
        return found

    students = [student_of(t) for t in range(T_LOCAL)]
    for t in range(T_LOCAL):
        student_table[t] = students[t]
        group_table[t] = jnp.where(students[t] >= GROUP, 1, 0)

    def prepare(t, _):
        q = tq[0, :, columns(t)]
        qy[t] = split_scaled(q)
        s = student_table[t]
        minus_q = jnp.zeros((ROWS, DH), jnp.bfloat16)
        for e in range(S_LOCAL):
            candidate = -sq[head, :, e * DH : (e + 1) * DH]
            minus_q = jnp.where(s == head * S_LOCAL + e, candidate, minus_q)
        qg[t] = jnp.concatenate([q, minus_q], axis=1)
        return 0

    lax.fori_loop(0, T_LOCAL, prepare, 0)
    other_lane = pl.multiple_of(384 - head * 128, 128)
    landed_s = remote(
        keys.at[kv, :, pl.ds(other_lane, 128)],
        keys.at[kv, :, pl.ds(other_lane, 128)],
        swap_send.at[0],
        swap_recv.at[0],
        partner,
    )
    landed_s.wait_recv()

    def z_copy(slot_row, c, send_sem, target_row):
        block = keys.at[slot_row * NX + col, pl.ds(c * CHUNK, CHUNK)]
        return remote(
            block, block, send_sem, z_recv.at[slot_row, c], device(dp, head, target_row * NX + col)
        )

    def up(c):
        return z_copy(row, c, z_send.at[0, c], row + 1)

    def down(c):
        return z_copy(row, c, z_send.at[1, c], (row + NZ - 1) % NZ)

    has_up = row < NZ - 1
    has_down = (row == 0, row < 2)

    def forward(slot_row, c):
        return z_copy(slot_row, c, relay_send.at[c], jnp.where(row == 0, NZ - 1, jnp.where(row == NZ - 1, 2, row + 1)))

    def x1(slot_row, c, side, target):
        block = keys.at[slot_row * NX + col, pl.ds(c * CHUNK, CHUNK)]
        return remote(
            block,
            block,
            x1_send.at[slot_row, c, side],
            x1_recv.at[slot_row, c, side],
            device(dp, head, target),
        )

    def x1_arrival(slot_row, c, side, source_col):
        block = keys.at[slot_row * NX + source_col, pl.ds(c * CHUNK, CHUNK)]
        return remote(
            block,
            block,
            x1_send.at[slot_row, c, side],
            x1_recv.at[slot_row, c, side],
            device(dp, head, right),
        )

    def x2(slot_row, c, side, source_col, target):
        block = keys.at[
            slot_row * NX + source_col, pl.ds(c * CHUNK + side * HALF, HALF)
        ]
        return remote(
            block,
            block,
            x2_send.at[slot_row, c, side],
            x2_recv.at[slot_row, c, side],
            device(dp, head, target),
        )

    def own_arrival(c, side, source_col):
        for part in range(2):
            block = keys.at[row * NX + source_col, pl.ds(c * CHUNK, CHUNK), pl.ds(256 * part, 256)]
            remote(
                block,
                block,
                own_send.at[c, side, part],
                own_recv.at[c, side, part],
                device(dp, head, right),
            ).wait_recv()

    left_col = (col + NX - 1) % NX
    right_col = (col + 1) % NX
    far_col = (col + 2) % NX

    def wave(w):
        early = w < 2
        last = row == NZ - 1
        k = w // 2
        r_last = jnp.where(w >= 6, 1, jnp.where(w % 2 == 0, 2, 0))
        c_last = jnp.where(w >= 6, w - 6, (w - 2) // 2)
        r = jnp.where(early, row, jnp.where(last, r_last, row - k))
        c = jnp.where(early, w, jnp.where(last, c_last, w % 2))
        return r, c

    def start_x1(r, c):
        x1(r, c, 0, right).start()
        x1(r, c, 1, left).start()

    def z_event(w):
        r, c = wave(w)
        z_copy(r, c, relay_send.at[c], row).wait_recv()
        start_x1(r, c)

        @pl.when(((row == NZ - 1) & (r == 0)) | ((row == 2) & (r == 1) & (c == 0)))
        def _():
            forward(r, c).start()

    def x_event(w):
        r, c = wave(w)
        x1_arrival(r, c, 0, left_col).wait_recv()
        x2(r, c, 0, left_col, right).start()
        x1_arrival(r, c, 1, right_col).wait_recv()
        x2(r, c, 1, right_col, left).start()

    def d_event(w):
        r, c = wave(w)
        x2(r, c, 0, far_col, right).wait_recv()
        x2(r, c, 1, far_col, right).wait_recv()

    def start_z(c):
        @pl.when(has_up)
        def _():
            up(c).start()

        @pl.when(has_down[c])
        def _():
            down(c).start()

    start_own(1)
    start_z(0)
    start_z(1)

    @pl.when(jnp.logical_not(last_row))
    def _():
        swap_q.start()

    waves = 2 * (row + 1)

    def events(event, *indices):
        for w in indices:

            @pl.when(w < waves)
            def _():
                event(w)

    def next_level(i):
        pl.semaphore_wait(levels.at[i - 1], len(near))
        greet_near(levels.at[i])

    def pieces_of(k):
        return wave(2 * k), wave(2 * k + 1)

    def tile(pieces, lane):
        return jnp.concatenate(
            [
                keys[pl.ds(r * NX, NX), pl.ds(c * CHUNK, CHUNK), pl.ds(lane, 128)].reshape(
                    PIECE, 128
                )
                for r, c in pieces
            ],
            axis=0,
        )

    def product(lhs, rhs):
        return lax.dot_general(lhs, rhs, NT, preferred_element_type=jnp.float32)

    def logits(pieces, t, lane, y_buf):
        k_t = tile(pieces, lane)
        y_buf[...] = product(jnp.concatenate([k_t, k_t], axis=1), qy[t])

    def student_products(pieces, t):
        k_s = tile(pieces, s_lane)
        y_s[...] = product(jnp.concatenate([k_s, k_s], axis=1), qs[t])

    def gaps(pieces, t, lane, g_buf):
        group = group_table[t]
        k_t = tile(pieces, lane)
        k_s = jnp.where(group == 0, tile(pieces, 256), tile(pieces, 384))
        g_buf[...] = product(jnp.concatenate([k_t, k_s], axis=1), qg[t])

    parts_of_tile = [pl.ds(n * SUB, SUB) for n in range(TILE // SUB)]

    def first_weights(y_buf, p_buf):
        def masked(part):
            return (y_buf[part] + bias[part]).reshape(SUB // 8, 8, ROWS)

        m = jnp.max(masked(parts_of_tile[0]), axis=0)
        for part in parts_of_tile[1:]:
            m = jnp.maximum(m, jnp.max(masked(part), axis=0))
        total = jnp.zeros((8, ROWS), jnp.float32)
        for part in parts_of_tile:
            p = jnp.exp2(masked(part) - m[None])
            total = total + jnp.sum(p, axis=0)
            if p_buf is not None:
                p_buf[part] = p.reshape(SUB, ROWS)
        return m, total

    def first_teacher(t, y_buf):
        m, total = first_weights(y_buf, first_p.at[t])
        t_state[t, 0:8] = m
        t_state[t, 8:16] = total

    def first_student(t):
        m, total = first_weights(y_s, None)
        s_state[t, 0:8] = m
        s_state[t, 8:16] = total

    def first_cross(t, g_buf):
        cross = jnp.zeros((8, ROWS), jnp.float32)
        for part in parts_of_tile:
            term = first_p[t, part] * g_buf[part]
            cross = cross + jnp.sum(term.reshape(SUB // 8, 8, ROWS), axis=0)
        t_state[t, 16:24] = cross

    own = pieces_of(0)

    def first_step(j, _):
        logits(own, GROUP + j, 128, y_b)
        student_products(own, j)
        first_teacher(j, y_a)
        logits(own, jnp.minimum(j + 1, GROUP - 1), 0, y_a)
        first_teacher(GROUP + j, y_b)
        first_student(j)
        return 0

    def cross_step(j, _):
        gaps(own, GROUP + j, 128, g_b)
        first_cross(j, g_a)
        gaps(own, j + 1, 0, g_a)
        first_cross(GROUP + j, g_b)
        return 0

    for c in range(2):
        own_arrival(c, 0, left_col)
        x2(row, c, 0, left_col, right).start()
        own_arrival(c, 1, right_col)
        x2(row, c, 1, right_col, left).start()
    next_level(1)
    events(z_event, 2)

    @pl.when(row == 0)
    def _():
        z_copy(1, 1, relay_send.at[1], row).wait_recv()
        forward(1, 1).start()

    events(z_event, 3)
    d_event(0)
    d_event(1)
    logits(own, 0, 0, y_a)
    lax.fori_loop(0, 4, first_step, 0)
    events(x_event, 2)
    lax.fori_loop(4, GROUP, first_step, 0)
    remote(sq.at[1 - head], sq.at[1 - head], swap_send.at[1], swap_recv.at[1], partner).wait_recv()
    events(x_event, 3)
    next_level(2)

    @pl.when(last_row)
    def _():
        events(z_event, 4, 5)

    def prepare_far(t, _):
        s = student_table[t]
        minus_q = qg[t, :, DH : 2 * DH]
        for e in range(S_LOCAL):
            candidate = -sq[1 - head, :, e * DH : (e + 1) * DH]
            minus_q = jnp.where(s == (1 - head) * S_LOCAL + e, candidate, minus_q)
        qg[t, :, DH : 2 * DH] = minus_q
        return 0

    lax.fori_loop(0, T_LOCAL, prepare_far, 0)

    def teacher_products(pieces, t, lane, y_buf, g_buf):
        group = group_table[t]
        k_t = tile(pieces, lane)
        k_s = jnp.where(group == 0, tile(pieces, 256), tile(pieces, 384))
        y_buf[...] = product(jnp.concatenate([k_t, k_t], axis=1), qy[t])
        g_buf[...] = product(jnp.concatenate([k_t, k_s], axis=1), qg[t])

    def weights(y_buf, part, running_max):
        y = y_buf[part].reshape(SUB // 8, 8, ROWS)
        new_max = jnp.maximum(running_max, jnp.max(y, axis=0))
        return new_max, jnp.exp2(running_max - new_max), jnp.exp2(y - new_max[None])

    def teacher_update(t, y_buf, g_buf):
        m, total, cross = t_state[t, 0:8], t_state[t, 8:16], t_state[t, 16:24]
        for part in parts_of_tile:
            m, rescale, p = weights(y_buf, part, m)
            total = total * rescale + jnp.sum(p, axis=0)
            cross = cross * rescale + jnp.sum(p * g_buf[part].reshape(p.shape), axis=0)
        t_state[t, 0:8] = m
        t_state[t, 8:16] = total
        t_state[t, 16:24] = cross

    def student_update(t):
        m, total = s_state[t, 0:8], s_state[t, 8:16]
        for part in parts_of_tile:
            m, rescale, p = weights(y_s, part, m)
            total = total * rescale + jnp.sum(p, axis=0)
        s_state[t, 0:8] = m
        s_state[t, 8:16] = total

    def step(now, after, j, _):
        final = j == GROUP - 1
        later = [
            tuple(jnp.where(final, new, old) for old, new in zip(*pair)) for pair in zip(now, after)
        ]
        teacher_products(now, GROUP + j, 128, y_b, g_b)
        student_products(now, j)
        teacher_update(j, y_a, g_a)
        teacher_products(later, jnp.where(final, 0, j + 1), 0, y_a, g_a)
        teacher_update(GROUP + j, y_b, g_b)
        student_update(j)
        return 0

    gaps(own, 0, 0, g_a)
    lax.fori_loop(0, GROUP - 1, cross_step, 0)
    events(d_event, 2, 3)
    gaps(own, T_LOCAL - 1, 128, g_b)
    first_cross(GROUP - 1, g_a)
    teacher_products(pieces_of(jnp.minimum(1, row)), 0, 0, y_a, g_a)
    first_cross(T_LOCAL - 1, g_b)
    next_level(3)

    def stretch(n, _):
        k = n // 3
        part = n % 3

        @pl.when((part == 0) & (k == 1) & jnp.logical_not(last_row))
        def _():
            events(z_event, 4, 5)

        @pl.when(part == 1)
        def _():
            events(x_event, 2 * k + 2, 2 * k + 3)
            events(z_event, 2 * k + 4, 2 * k + 5)

        @pl.when(part == 2)
        def _():
            events(d_event, 2 * k + 2, 2 * k + 3)

        lax.fori_loop(
            jnp.where(part == 0, 0, jnp.where(part == 1, 2, 6)),
            jnp.where(part == 0, 2, jnp.where(part == 1, 6, GROUP)),
            functools.partial(step, pieces_of(k), pieces_of(jnp.minimum(k + 1, row))),
            0,
        )
        return 0

    lax.fori_loop(3, 3 * (row + 1), stretch, 0)

    lane_row = lax.broadcasted_iota(jnp.int32, (8, ROWS), 0)
    parts = [jnp.zeros((8, ROWS), jnp.float32), jnp.zeros((8, ROWS), jnp.float32)]
    for t in range(T_LOCAL):
        m = t_state[t, 0:8]
        top = jnp.max(m, axis=0, keepdims=True)
        w = jnp.exp2(m - top)
        total = jnp.sum(t_state[t, 8:16] * w, axis=0, keepdims=True)
        cross = jnp.sum(t_state[t, 16:24] * w, axis=0, keepdims=True)
        value = cross / total * SCALE - (top + jnp.log2(total)) * LN2
        for g in range(2):
            parts[g] = parts[g] + jnp.where(lane_row == students[t] - g * GROUP, value, 0.0) * jnp.where(
                (students[t] >= GROUP) == (g == 1), 1.0, 0.0
            )
    home = jnp.zeros((8, ROWS), jnp.float32)
    for t in range(S_LOCAL):
        m = s_state[t, 0:8]
        top = jnp.max(m, axis=0, keepdims=True)
        total = jnp.sum(s_state[t, 8:16] * jnp.exp2(m - top), axis=0, keepdims=True)
        home = home + jnp.where(lane_row == t, (top + jnp.log2(total)) * (2.0 * LN2), 0.0)
    for g in range(2):
        contrib[g] = parts[g] + jnp.where(head == g, home, 0.0)
    pl.semaphore_wait(levels.at[3], len(near))
    kl_copy = remote(contrib.at[1 - head], kl_other, kl_sem.at[0], kl_sem.at[1], partner)
    kl_copy.start()

    me = head * N_KV + kv
    for g in range(2):
        block = jnp.sum(contrib[g], axis=1, keepdims=True)
        sums_plane[2 * N_KV + g] = jnp.broadcast_to(block, (8, 128))

    def plane_copy(i):
        peer = (me + i) % (2 * N_KV)
        return remote(
            sums_plane.at[2 * N_KV + peer // N_KV],
            sums_plane.at[me],
            plane_send.at[i],
            plane_recv.at[me],
            device(dp, peer // N_KV, peer % N_KV),
        )

    def plane_start(i, _):
        plane_copy(i).start()
        return 0

    lax.fori_loop(1, 2 * N_KV, plane_start, 0)

    kl_copy.wait()
    kl_out[0] = (contrib[head] + kl_other[...])[0:S_LOCAL]

    def plane_wait(i, total):
        source = (me + i) % (2 * N_KV)
        remote(
            sums_plane.at[source],
            sums_plane.at[source],
            plane_send.at[i],
            plane_recv.at[source],
            partner,
        ).wait_recv()
        return total + sums_plane[source]

    plane_total = lax.fori_loop(1, 2 * N_KV, plane_wait, sums_plane[2 * N_KV + head])
    sums_dp[N_DP] = plane_total

    def dp_copy(i):
        return remote(
            sums_dp.at[N_DP],
            sums_dp.at[dp],
            dp_send.at[i],
            dp_recv.at[dp],
            device((dp + i) % N_DP, head, kv),
        )

    for i in range(1, N_DP):
        dp_copy(i).start()
    grand = plane_total
    for i in range(1, N_DP):
        source = (dp + i) % N_DP
        remote(
            sums_dp.at[source], sums_dp.at[source], dp_send.at[i], dp_recv.at[source], partner
        ).wait_recv()
        grand = grand + sums_dp[source]
    loss_out[...] = grand * (1.0 / (N_DP * N_KV * ROWS))

    swap_s.wait_send()
    swap_q.wait_send()
    for c in range(2):

        @pl.when(has_up)
        def _():
            up(c).wait_send()

        @pl.when(has_down[c])
        def _():
            down(c).wait_send()

        @pl.when(row == NZ - 1)
        def _():
            forward(0, c).wait_send()

    @pl.when(row == 0)
    def _():
        forward(1, 1).wait_send()

    @pl.when(row == 2)
    def _():
        forward(1, 0).wait_send()

    for c in range(2):
        for part in range(2):
            own_part(c, 0, part, right).wait_send()
            own_part(c, 1, part, left).wait_send()

    def drain(w, _):
        r, c = wave(w)

        @pl.when(w > 1)
        def _():
            x1(r, c, 0, right).wait_send()
            x1(r, c, 1, left).wait_send()

        x2(r, c, 0, left_col, right).wait_send()
        x2(r, c, 1, right_col, left).wait_send()
        return 0

    lax.fori_loop(0, waves, drain, 0)

    def plane_drain(i, _):
        plane_copy(i).wait_send()
        return 0

    lax.fori_loop(1, 2 * N_KV, plane_drain, 0)
    for i in range(1, N_DP):
        dp_copy(i).wait_send()


def per_device(teacher_query, teacher_key, student_query, student_key, pair_table):
    vmem = pl.BlockSpec(memory_space=pltpu.VMEM)
    anywhere = pl.BlockSpec(memory_space=pl.ANY)
    dma = pltpu.SemaphoreType.DMA
    f32, bf16 = jnp.float32, jnp.bfloat16
    kl, loss = pl.pallas_call(
        kernel,
        out_shape=(
            jax.ShapeDtypeStruct((1, S_LOCAL, ROWS), f32),
            jax.ShapeDtypeStruct((8, 128), f32),
        ),
        in_specs=[pl.BlockSpec(memory_space=pltpu.SMEM), vmem, anywhere, anywhere, anywhere],
        out_specs=(vmem, vmem),
        scratch_shapes=[
            pltpu.VMEM((N_KV, ROWS, 512), bf16),
            pltpu.VMEM((2, ROWS, S_LOCAL * DH), bf16),
            pltpu.VMEM((T_LOCAL, ROWS, 256), bf16),
            pltpu.VMEM((T_LOCAL, ROWS, 256), bf16),
            pltpu.VMEM((S_LOCAL, ROWS, 256), bf16),
            pltpu.VMEM((T_LOCAL, 24, ROWS), f32),
            pltpu.VMEM((S_LOCAL, 16, ROWS), f32),
            pltpu.VMEM((TILE, ROWS), f32),
            pltpu.VMEM((TILE, ROWS), f32),
            pltpu.VMEM((TILE, ROWS), f32),
            pltpu.VMEM((TILE, ROWS), f32),
            pltpu.VMEM((TILE, ROWS), f32),
            pltpu.VMEM((T_LOCAL, TILE, ROWS), f32),
            pltpu.VMEM((TILE, ROWS), f32),
            pltpu.VMEM((2, 8, ROWS), f32),
            pltpu.VMEM((8, ROWS), f32),
            pltpu.VMEM((2 * N_KV + 2, 8, 128), f32),
            pltpu.VMEM((N_DP + 1, 8, 128), f32),
            pltpu.SMEM((T_LOCAL,), jnp.int32),
            pltpu.SMEM((T_LOCAL,), jnp.int32),
            pltpu.SemaphoreType.REGULAR((4,)),
            dma((3,)),
            dma((2,)),
            dma((2,)),
            dma((2, 2)),
            dma((NZ, 2)),
            dma((2,)),
            dma((NZ, 2, 2)),
            dma((NZ, 2, 2)),
            dma((NZ, 2, 2)),
            dma((NZ, 2, 2)),
            dma((2, 2, 2)),
            dma((2, 2, 2)),
            dma((2,)),
            dma((2 * N_KV,)),
            dma((2 * N_KV,)),
            dma((N_DP,)),
            dma((N_DP,)),
        ],
        compiler_params=pltpu.CompilerParams(
            collective_id=0, has_side_effects=True, vmem_limit_bytes=60 * 1024 * 1024
        ),
    )(pair_table, teacher_query, teacher_key, student_query, student_key)
    return kl, loss[:S_LOCAL, 0]


def solution(mesh):
    spec = P("dp", "kv", "head")
    return jax.shard_map(
        per_device,
        mesh=mesh,
        in_specs=(spec, spec, spec, spec, P()),
        out_specs=(P("dp", "head", "kv"), P("head")),
        check_vma=False,
    )
```

```python
import functools
import math

import jax
import jax.numpy as jnp
from jax import lax
from jax.experimental import pallas as pl
from jax.experimental.pallas import tpu as pltpu
from jax.sharding import PartitionSpec as P

HT = 28
HS = 14
DH = 128
GROUP = 7
NX = 4
NZ = 4
N_KV = NX * NZ
N_DP = 8
ROWS = 256
CHUNK = 128
HALF = CHUNK // 2
PIECE = NX * CHUNK
TILE = 2 * PIECE
SUB = 128
T_LOCAL = 14
S_LOCAL = 7
SCALE = 1.0 / math.sqrt(DH)
LOG2E = math.log2(math.e)
LN2 = math.log(2.0)
NEG = -1e30
MESH = pl.DeviceIdType.MESH
NT = (((1,), (1,)), ((), ()))


def split_scaled(q):
    scaled = q.astype(jnp.float32) * (SCALE * LOG2E)
    hi = scaled.astype(jnp.bfloat16)
    lo = (scaled - hi.astype(jnp.float32)).astype(jnp.bfloat16)
    return jnp.concatenate([hi, lo], axis=1)


def kernel(
    table,
    tq_in,
    tk_in,
    sq_in,
    sk_in,
    kl_out,
    loss_out,
    keys,
    tq,
    sq,
    qy,
    qg,
    qs,
    t_state,
    s_state,
    y_a,
    g_a,
    y_b,
    g_b,
    y_s,
    first_p,
    bias,
    contrib,
    kl_other,
    sums_plane,
    sums_dp,
    group_table,
    student_table,
    levels,
    local_sem,
    swap_send,
    swap_recv,
    z_send,
    z_recv,
    relay_send,
    x1_send,
    x1_recv,
    x2_send,
    x2_recv,
    own_send,
    own_recv,
    kl_sem,
    plane_send,
    plane_recv,
    dp_send,
    dp_recv,
):
    dp = lax.axis_index("dp")
    head = lax.axis_index("head")
    kv = lax.axis_index("kv")
    row = kv // NX
    col = kv % NX
    right = row * NX + (col + 1) % NX
    left = row * NX + (col + NX - 1) % NX

    def device(d, h, k):
        return (d, h, k)

    def remote(src, dst, send_sem, recv_sem, dev):
        return pltpu.make_async_remote_copy(
            src_ref=src,
            dst_ref=dst,
            send_sem=send_sem,
            recv_sem=recv_sem,
            device_id=dev,
            device_id_type=MESH,
        )

    s_lane = pl.multiple_of(256 + head * 128, 128)
    fill_t = pltpu.make_async_copy(tk_in.at[0], keys.at[kv, :, pl.ds(0, 256)], local_sem.at[0])
    fill_s = pltpu.make_async_copy(sk_in.at[0], keys.at[kv, :, pl.ds(s_lane, 128)], local_sem.at[1])
    fill_q = pltpu.make_async_copy(sq_in.at[0], sq.at[head], local_sem.at[2])
    fill_tq = pltpu.make_async_copy(tq_in.at[0], tq, local_sem.at[3])
    fill_s.start()
    fill_t.start()
    fill_q.start()
    fill_tq.start()

    partner = device(dp, 1 - head, kv)
    near = (
        partner,
        device(dp, head, right),
        device(dp, head, left),
        device(dp, head, (kv + NX) % N_KV),
        device(dp, head, (kv + N_KV - NX) % N_KV),
    )
    barrier = pltpu.get_barrier_semaphore()

    def greet_near(semaphore):
        for peer in near:
            pl.semaphore_signal(semaphore, inc=1, device_id=peer, device_id_type=MESH)

    greet_near(barrier)
    for i in range(1, N_DP):
        pl.semaphore_signal(
            barrier, inc=1, device_id=device((dp + i) % N_DP, head, kv), device_id_type=MESH
        )

    def columns(h):
        return pl.ds(pl.multiple_of(h * DH, DH), DH)

    fill_q.wait()

    def prepare_student(t, _):
        qs[t] = split_scaled(sq[head, :, columns(t)])
        return 0

    lax.fori_loop(0, S_LOCAL, prepare_student, 0)
    bias_col = col * ROWS + lax.broadcasted_iota(jnp.int32, (PIECE, ROWS), 1)
    bias_pos = lax.broadcasted_iota(jnp.int32, (PIECE, ROWS), 0)
    bias_key = bias_pos + (bias_pos // CHUNK) * (ROWS - CHUNK)
    for c in range(2):
        bias[c * PIECE : (c + 1) * PIECE] = jnp.where(bias_key + c * CHUNK <= bias_col, 0.0, NEG)
    fill_s.wait()
    fill_t.wait()
    pl.semaphore_wait(barrier, len(near) + N_DP - 1)

    def own_part(c, side, part, target):
        block = keys.at[kv, pl.ds(c * CHUNK, CHUNK), pl.ds(256 * part, 256)]
        return remote(
            block, block, own_send.at[c, side, part], own_recv.at[c, side, part], device(dp, head, target)
        )

    def start_own(part):
        for c in range(2):
            own_part(c, 0, part, right).start()
            own_part(c, 1, part, left).start()

    swap_s = remote(
        keys.at[kv, :, pl.ds(s_lane, 128)],
        keys.at[kv, :, pl.ds(s_lane, 128)],
        swap_send.at[0],
        swap_recv.at[0],
        partner,
    )
    swap_s.start()
    start_own(0)
    greet_near(levels.at[0])
    swap_q = remote(sq.at[head], sq.at[head], swap_send.at[1], swap_recv.at[1], partner)
    last_row = row == NZ - 1

    @pl.when(last_row)
    def _():
        swap_q.start()


    def student_of(t):
        found = jnp.int32(0)
        for e in range(HT):
            found = jnp.where(table[e % 2, e // 2] == head * T_LOCAL + t, e // 2, found)
        return found

    students = [student_of(t) for t in range(T_LOCAL)]
    for t in range(T_LOCAL):
        student_table[t] = students[t]
        group_table[t] = jnp.where(students[t] >= GROUP, 1, 0)

    def prepare(t, _):
        q = tq[:, columns(t)]
        qy[t] = split_scaled(q)
        s = student_table[t]
        minus_q = jnp.zeros((ROWS, DH), jnp.bfloat16)
        for e in range(S_LOCAL):
            candidate = -sq[head, :, e * DH : (e + 1) * DH]
            minus_q = jnp.where(s == head * S_LOCAL + e, candidate, minus_q)
        qg[t] = jnp.concatenate([q, minus_q], axis=1)
        return 0

    fill_tq.wait()
    lax.fori_loop(0, T_LOCAL, prepare, 0)
    other_lane = pl.multiple_of(384 - head * 128, 128)
    landed_s = remote(
        keys.at[kv, :, pl.ds(other_lane, 128)],
        keys.at[kv, :, pl.ds(other_lane, 128)],
        swap_send.at[0],
        swap_recv.at[0],
        partner,
    )
    landed_s.wait_recv()

    def z_copy(slot_row, c, send_sem, target_row):
        block = keys.at[slot_row * NX + col, pl.ds(c * CHUNK, CHUNK)]
        return remote(
            block, block, send_sem, z_recv.at[slot_row, c], device(dp, head, target_row * NX + col)
        )

    def up(c):
        return z_copy(row, c, z_send.at[0, c], row + 1)

    def down(c):
        return z_copy(row, c, z_send.at[1, c], (row + NZ - 1) % NZ)

    has_up = row < NZ - 1
    has_down = (row == 0, row < 2)

    def forward(slot_row, c):
        return z_copy(slot_row, c, relay_send.at[c], jnp.where(row == 0, NZ - 1, jnp.where(row == NZ - 1, 2, row + 1)))

    def x1(slot_row, c, side, target):
        block = keys.at[slot_row * NX + col, pl.ds(c * CHUNK, CHUNK)]
        return remote(
            block,
            block,
            x1_send.at[slot_row, c, side],
            x1_recv.at[slot_row, c, side],
            device(dp, head, target),
        )

    def x1_arrival(slot_row, c, side, source_col):
        block = keys.at[slot_row * NX + source_col, pl.ds(c * CHUNK, CHUNK)]
        return remote(
            block,
            block,
            x1_send.at[slot_row, c, side],
            x1_recv.at[slot_row, c, side],
            device(dp, head, right),
        )

    def x2(slot_row, c, side, source_col, target):
        block = keys.at[
            slot_row * NX + source_col, pl.ds(c * CHUNK + side * HALF, HALF)
        ]
        return remote(
            block,
            block,
            x2_send.at[slot_row, c, side],
            x2_recv.at[slot_row, c, side],
            device(dp, head, target),
        )

    def own_arrival(c, side, source_col):
        for part in range(2):
            block = keys.at[row * NX + source_col, pl.ds(c * CHUNK, CHUNK), pl.ds(256 * part, 256)]
            remote(
                block,
                block,
                own_send.at[c, side, part],
                own_recv.at[c, side, part],
                device(dp, head, right),
            ).wait_recv()

    left_col = (col + NX - 1) % NX
    right_col = (col + 1) % NX
    far_col = (col + 2) % NX

    def wave(w):
        early = w < 2
        last = row == NZ - 1
        k = w // 2
        r_last = jnp.where(w >= 6, 1, jnp.where(w % 2 == 0, 2, 0))
        c_last = jnp.where(w >= 6, w - 6, (w - 2) // 2)
        r = jnp.where(early, row, jnp.where(last, r_last, row - k))
        c = jnp.where(early, w, jnp.where(last, c_last, w % 2))
        return r, c

    def start_x1(r, c):
        x1(r, c, 0, right).start()
        x1(r, c, 1, left).start()

    def z_event(w):
        r, c = wave(w)
        z_copy(r, c, relay_send.at[c], row).wait_recv()
        start_x1(r, c)

        @pl.when(((row == NZ - 1) & (r == 0)) | ((row == 2) & (r == 1) & (c == 0)))
        def _():
            forward(r, c).start()

    def x_event(w):
        r, c = wave(w)
        x1_arrival(r, c, 0, left_col).wait_recv()
        x2(r, c, 0, left_col, right).start()
        x1_arrival(r, c, 1, right_col).wait_recv()
        x2(r, c, 1, right_col, left).start()

    def d_event(w):
        r, c = wave(w)
        x2(r, c, 0, far_col, right).wait_recv()
        x2(r, c, 1, far_col, right).wait_recv()

    def start_z(c):
        @pl.when(has_up)
        def _():
            up(c).start()

        @pl.when(has_down[c])
        def _():
            down(c).start()

    start_own(1)
    start_z(0)
    start_z(1)

    @pl.when(jnp.logical_not(last_row))
    def _():
        swap_q.start()

    waves = 2 * (row + 1)

    def events(event, *indices):
        for w in indices:

            @pl.when(w < waves)
            def _():
                event(w)

    def next_level(i):
        pl.semaphore_wait(levels.at[i - 1], len(near))
        greet_near(levels.at[i])

    def pieces_of(k):
        return wave(2 * k), wave(2 * k + 1)

    def tile(pieces, lane):
        return jnp.concatenate(
            [
                keys[pl.ds(r * NX, NX), pl.ds(c * CHUNK, CHUNK), pl.ds(lane, 128)].reshape(
                    PIECE, 128
                )
                for r, c in pieces
            ],
            axis=0,
        )

    def product(lhs, rhs):
        return lax.dot_general(lhs, rhs, NT, preferred_element_type=jnp.float32)

    def logits(pieces, t, lane, y_buf):
        k_t = tile(pieces, lane)
        y_buf[...] = product(jnp.concatenate([k_t, k_t], axis=1), qy[t])

    def student_products(pieces, t):
        k_s = tile(pieces, s_lane)
        y_s[...] = product(jnp.concatenate([k_s, k_s], axis=1), qs[t])

    def gaps(pieces, t, lane, g_buf):
        group = group_table[t]
        k_t = tile(pieces, lane)
        k_s = jnp.where(group == 0, tile(pieces, 256), tile(pieces, 384))
        g_buf[...] = product(jnp.concatenate([k_t, k_s], axis=1), qg[t])

    parts_of_tile = [pl.ds(n * SUB, SUB) for n in range(TILE // SUB)]

    def first_weights(y_buf, p_buf):
        def masked(part):
            return (y_buf[part] + bias[part]).reshape(SUB // 8, 8, ROWS)

        m = jnp.max(masked(parts_of_tile[0]), axis=0)
        for part in parts_of_tile[1:]:
            m = jnp.maximum(m, jnp.max(masked(part), axis=0))
        total = jnp.zeros((8, ROWS), jnp.float32)
        for part in parts_of_tile:
            p = jnp.exp2(masked(part) - m[None])
            total = total + jnp.sum(p, axis=0)
            if p_buf is not None:
                p_buf[part] = p.reshape(SUB, ROWS)
        return m, total

    def first_teacher(t, y_buf):
        m, total = first_weights(y_buf, first_p.at[t])
        t_state[t, 0:8] = m
        t_state[t, 8:16] = total

    def first_student(t):
        m, total = first_weights(y_s, None)
        s_state[t, 0:8] = m
        s_state[t, 8:16] = total

    def first_cross(t, g_buf):
        cross = jnp.zeros((8, ROWS), jnp.float32)
        for part in parts_of_tile:
            term = first_p[t, part] * g_buf[part]
            cross = cross + jnp.sum(term.reshape(SUB // 8, 8, ROWS), axis=0)
        t_state[t, 16:24] = cross

    own = pieces_of(0)

    def first_step(j, _):
        logits(own, GROUP + j, 128, y_b)
        student_products(own, j)
        first_teacher(j, y_a)
        logits(own, jnp.minimum(j + 1, GROUP - 1), 0, y_a)
        first_teacher(GROUP + j, y_b)
        first_student(j)
        return 0

    def cross_step(j, _):
        gaps(own, GROUP + j, 128, g_b)
        first_cross(j, g_a)
        gaps(own, j + 1, 0, g_a)
        first_cross(GROUP + j, g_b)
        return 0

    for c in range(2):
        own_arrival(c, 0, left_col)
        x2(row, c, 0, left_col, right).start()
        own_arrival(c, 1, right_col)
        x2(row, c, 1, right_col, left).start()
    next_level(1)
    events(z_event, 2)

    @pl.when(row == 0)
    def _():
        z_copy(1, 1, relay_send.at[1], row).wait_recv()
        forward(1, 1).start()

    events(z_event, 3)
    d_event(0)
    d_event(1)
    logits(own, 0, 0, y_a)
    lax.fori_loop(0, 3, first_step, 0)
    events(x_event, 2)
    lax.fori_loop(3, 5, first_step, 0)
    events(x_event, 3)

    @pl.when(last_row)
    def _():
        events(z_event, 4, 5)

    lax.fori_loop(5, GROUP, first_step, 0)
    remote(sq.at[1 - head], sq.at[1 - head], swap_send.at[1], swap_recv.at[1], partner).wait_recv()
    next_level(2)

    def prepare_far(t, _):
        s = student_table[t]
        minus_q = qg[t, :, DH : 2 * DH]
        for e in range(S_LOCAL):
            candidate = -sq[1 - head, :, e * DH : (e + 1) * DH]
            minus_q = jnp.where(s == (1 - head) * S_LOCAL + e, candidate, minus_q)
        qg[t, :, DH : 2 * DH] = minus_q
        return 0

    lax.fori_loop(0, T_LOCAL, prepare_far, 0)

    def teacher_products(pieces, t, lane, y_buf, g_buf):
        group = group_table[t]
        k_t = tile(pieces, lane)
        k_s = jnp.where(group == 0, tile(pieces, 256), tile(pieces, 384))
        y_buf[...] = product(jnp.concatenate([k_t, k_t], axis=1), qy[t])
        g_buf[...] = product(jnp.concatenate([k_t, k_s], axis=1), qg[t])

    def weights(y_buf, part, running_max):
        y = y_buf[part].reshape(SUB // 8, 8, ROWS)
        new_max = jnp.maximum(running_max, jnp.max(y, axis=0))
        return new_max, jnp.exp2(running_max - new_max), jnp.exp2(y - new_max[None])

    def teacher_update(t, y_buf, g_buf):
        m, total, cross = t_state[t, 0:8], t_state[t, 8:16], t_state[t, 16:24]
        for part in parts_of_tile:
            m, rescale, p = weights(y_buf, part, m)
            total = total * rescale + jnp.sum(p, axis=0)
            cross = cross * rescale + jnp.sum(p * g_buf[part].reshape(p.shape), axis=0)
        t_state[t, 0:8] = m
        t_state[t, 8:16] = total
        t_state[t, 16:24] = cross

    def student_update(t):
        m, total = s_state[t, 0:8], s_state[t, 8:16]
        for part in parts_of_tile:
            m, rescale, p = weights(y_s, part, m)
            total = total * rescale + jnp.sum(p, axis=0)
        s_state[t, 0:8] = m
        s_state[t, 8:16] = total

    def step(now, after, j, _):
        final = j == GROUP - 1
        later = [
            tuple(jnp.where(final, new, old) for old, new in zip(*pair)) for pair in zip(now, after)
        ]
        teacher_products(now, GROUP + j, 128, y_b, g_b)
        student_products(now, j)
        teacher_update(j, y_a, g_a)
        teacher_products(later, jnp.where(final, 0, j + 1), 0, y_a, g_a)
        teacher_update(GROUP + j, y_b, g_b)
        student_update(j)
        return 0

    gaps(own, 0, 0, g_a)
    lax.fori_loop(0, GROUP - 1, cross_step, 0)
    events(d_event, 2, 3)
    gaps(own, T_LOCAL - 1, 128, g_b)
    first_cross(GROUP - 1, g_a)
    teacher_products(pieces_of(jnp.minimum(1, row)), 0, 0, y_a, g_a)
    first_cross(T_LOCAL - 1, g_b)
    next_level(3)

    def stretch(n, _):
        k = n // 3
        part = n % 3

        @pl.when((part == 0) & (k == 1) & jnp.logical_not(last_row))
        def _():
            events(z_event, 4, 5)

        @pl.when(part == jnp.where(last_row & (k == 1), 0, 1))
        def _():
            events(x_event, 2 * k + 2, 2 * k + 3)
            events(z_event, 2 * k + 4, 2 * k + 5)

        @pl.when(part == 2)
        def _():
            events(d_event, 2 * k + 2, 2 * k + 3)

        lax.fori_loop(
            jnp.where(part == 0, 0, jnp.where(part == 1, 2, 6)),
            jnp.where(part == 0, 2, jnp.where(part == 1, 6, GROUP)),
            functools.partial(step, pieces_of(k), pieces_of(jnp.minimum(k + 1, row))),
            0,
        )
        return 0

    lax.fori_loop(3, 3 * (row + 1), stretch, 0)

    lane_row = lax.broadcasted_iota(jnp.int32, (8, ROWS), 0)
    parts = [jnp.zeros((8, ROWS), jnp.float32), jnp.zeros((8, ROWS), jnp.float32)]
    for t in range(T_LOCAL):
        m = t_state[t, 0:8]
        top = jnp.max(m, axis=0, keepdims=True)
        w = jnp.exp2(m - top)
        total = jnp.sum(t_state[t, 8:16] * w, axis=0, keepdims=True)
        cross = jnp.sum(t_state[t, 16:24] * w, axis=0, keepdims=True)
        value = cross / total * SCALE - (top + jnp.log2(total)) * LN2
        for g in range(2):
            parts[g] = parts[g] + jnp.where(lane_row == students[t] - g * GROUP, value, 0.0) * jnp.where(
                (students[t] >= GROUP) == (g == 1), 1.0, 0.0
            )
    home = jnp.zeros((8, ROWS), jnp.float32)
    for t in range(S_LOCAL):
        m = s_state[t, 0:8]
        top = jnp.max(m, axis=0, keepdims=True)
        total = jnp.sum(s_state[t, 8:16] * jnp.exp2(m - top), axis=0, keepdims=True)
        home = home + jnp.where(lane_row == t, (top + jnp.log2(total)) * (2.0 * LN2), 0.0)
    for g in range(2):
        contrib[g] = parts[g] + jnp.where(head == g, home, 0.0)
    pl.semaphore_wait(levels.at[3], len(near))
    kl_copy = remote(contrib.at[1 - head], kl_other, kl_sem.at[0], kl_sem.at[1], partner)
    kl_copy.start()

    me = head * N_KV + kv
    for g in range(2):
        block = jnp.sum(contrib[g], axis=1, keepdims=True)
        sums_plane[2 * N_KV + g] = jnp.broadcast_to(block, (8, 128))

    def plane_copy(i):
        peer = (me + i) % (2 * N_KV)
        return remote(
            sums_plane.at[2 * N_KV + peer // N_KV],
            sums_plane.at[me],
            plane_send.at[i],
            plane_recv.at[me],
            device(dp, peer // N_KV, peer % N_KV),
        )

    def plane_start(i, _):
        plane_copy(i).start()
        return 0

    lax.fori_loop(1, 2 * N_KV, plane_start, 0)

    kl_copy.wait()
    kl_rows = contrib[head] + kl_other[...]
    for t in range(S_LOCAL):
        kl_out[t] = kl_rows[t : t + 1]

    def plane_wait(i, total):
        source = (me + i) % (2 * N_KV)
        remote(
            sums_plane.at[source],
            sums_plane.at[source],
            plane_send.at[i],
            plane_recv.at[source],
            partner,
        ).wait_recv()
        return total + sums_plane[source]

    plane_total = lax.fori_loop(1, 2 * N_KV, plane_wait, sums_plane[2 * N_KV + head])
    sums_dp[N_DP] = plane_total

    def dp_copy(i):
        return remote(
            sums_dp.at[N_DP],
            sums_dp.at[dp],
            dp_send.at[i],
            dp_recv.at[dp],
            device((dp + i) % N_DP, head, kv),
        )

    for i in range(1, N_DP):
        dp_copy(i).start()
    grand = plane_total
    for i in range(1, N_DP):
        source = (dp + i) % N_DP
        remote(
            sums_dp.at[source], sums_dp.at[source], dp_send.at[i], dp_recv.at[source], partner
        ).wait_recv()
        grand = grand + sums_dp[source]
    loss_out[...] = grand * (1.0 / (N_DP * N_KV * ROWS))

    swap_s.wait_send()
    swap_q.wait_send()
    for c in range(2):

        @pl.when(has_up)
        def _():
            up(c).wait_send()

        @pl.when(has_down[c])
        def _():
            down(c).wait_send()

        @pl.when(row == NZ - 1)
        def _():
            forward(0, c).wait_send()

    @pl.when(row == 0)
    def _():
        forward(1, 1).wait_send()

    @pl.when(row == 2)
    def _():
        forward(1, 0).wait_send()

    for c in range(2):
        for part in range(2):
            own_part(c, 0, part, right).wait_send()
            own_part(c, 1, part, left).wait_send()

    def drain(w, _):
        r, c = wave(w)

        @pl.when(w > 1)
        def _():
            x1(r, c, 0, right).wait_send()
            x1(r, c, 1, left).wait_send()

        x2(r, c, 0, left_col, right).wait_send()
        x2(r, c, 1, right_col, left).wait_send()
        return 0

    lax.fori_loop(0, waves, drain, 0)

    def plane_drain(i, _):
        plane_copy(i).wait_send()
        return 0

    lax.fori_loop(1, 2 * N_KV, plane_drain, 0)
    for i in range(1, N_DP):
        dp_copy(i).wait_send()


def per_device(teacher_query, teacher_key, student_query, student_key, pair_table):
    vmem = pl.BlockSpec(memory_space=pltpu.VMEM)
    anywhere = pl.BlockSpec(memory_space=pl.ANY)
    dma = pltpu.SemaphoreType.DMA
    f32, bf16 = jnp.float32, jnp.bfloat16
    kl, loss = pl.pallas_call(
        kernel,
        out_shape=(
            jax.ShapeDtypeStruct((S_LOCAL, 1, ROWS), f32),
            jax.ShapeDtypeStruct((8, 128), f32),
        ),
        in_specs=[pl.BlockSpec(memory_space=pltpu.SMEM), anywhere, anywhere, anywhere, anywhere],
        out_specs=(vmem, vmem),
        scratch_shapes=[
            pltpu.VMEM((N_KV, ROWS, 512), bf16),
            pltpu.VMEM((ROWS, T_LOCAL * DH), bf16),
            pltpu.VMEM((2, ROWS, S_LOCAL * DH), bf16),
            pltpu.VMEM((T_LOCAL, ROWS, 256), bf16),
            pltpu.VMEM((T_LOCAL, ROWS, 256), bf16),
            pltpu.VMEM((S_LOCAL, ROWS, 256), bf16),
            pltpu.VMEM((T_LOCAL, 24, ROWS), f32),
            pltpu.VMEM((S_LOCAL, 16, ROWS), f32),
            pltpu.VMEM((TILE, ROWS), f32),
            pltpu.VMEM((TILE, ROWS), f32),
            pltpu.VMEM((TILE, ROWS), f32),
            pltpu.VMEM((TILE, ROWS), f32),
            pltpu.VMEM((TILE, ROWS), f32),
            pltpu.VMEM((T_LOCAL, TILE, ROWS), f32),
            pltpu.VMEM((TILE, ROWS), f32),
            pltpu.VMEM((2, 8, ROWS), f32),
            pltpu.VMEM((8, ROWS), f32),
            pltpu.VMEM((2 * N_KV + 2, 8, 128), f32),
            pltpu.VMEM((N_DP + 1, 8, 128), f32),
            pltpu.SMEM((T_LOCAL,), jnp.int32),
            pltpu.SMEM((T_LOCAL,), jnp.int32),
            pltpu.SemaphoreType.REGULAR((4,)),
            dma((4,)),
            dma((2,)),
            dma((2,)),
            dma((2, 2)),
            dma((NZ, 2)),
            dma((2,)),
            dma((NZ, 2, 2)),
            dma((NZ, 2, 2)),
            dma((NZ, 2, 2)),
            dma((NZ, 2, 2)),
            dma((2, 2, 2)),
            dma((2, 2, 2)),
            dma((2,)),
            dma((2 * N_KV,)),
            dma((2 * N_KV,)),
            dma((N_DP,)),
            dma((N_DP,)),
        ],
        compiler_params=pltpu.CompilerParams(
            collective_id=0, has_side_effects=True, vmem_limit_bytes=60 * 1024 * 1024
        ),
    )(pair_table.T, teacher_query, teacher_key, student_query, student_key)
    return jnp.transpose(kl, (1, 0, 2)), loss[:S_LOCAL, 0]


def solution(mesh):
    spec = P("dp", "kv", "head")
    return jax.shard_map(
        per_device,
        mesh=mesh,
        in_specs=(spec, spec, spec, spec, P()),
        out_specs=(P("dp", "head", "kv"), P("head")),
        check_vma=False,
    )
```

```python
import functools
import math

import jax
import jax.numpy as jnp
from jax import lax
from jax.experimental import pallas as pl
from jax.experimental.pallas import tpu as pltpu
from jax.sharding import PartitionSpec as P

HT = 28
HS = 14
DH = 128
GROUP = 7
NX = 4
NZ = 4
N_KV = NX * NZ
N_DP = 8
ROWS = 256
CHUNK = 128
HALF = CHUNK // 2
PIECE = NX * CHUNK
TILE = 2 * PIECE
SUB = 128
T_LOCAL = 14
S_LOCAL = 7
SCALE = 1.0 / math.sqrt(DH)
LOG2E = math.log2(math.e)
LN2 = math.log(2.0)
NEG = -1e30
MESH = pl.DeviceIdType.MESH
NT = (((1,), (1,)), ((), ()))


def split_scaled(q):
    scaled = q.astype(jnp.float32) * (SCALE * LOG2E)
    hi = scaled.astype(jnp.bfloat16)
    lo = (scaled - hi.astype(jnp.float32)).astype(jnp.bfloat16)
    return jnp.concatenate([hi, lo], axis=1)


def kernel(
    table,
    tq_in,
    tk_in,
    sq_in,
    sk_in,
    kl_out,
    loss_out,
    keys,
    tq,
    sq,
    qy,
    qg,
    qs,
    t_state,
    s_state,
    y_a,
    g_a,
    y_b,
    g_b,
    y_s,
    first_p,
    bias,
    contrib,
    kl_other,
    sums_plane,
    sums_dp,
    group_table,
    student_table,
    levels,
    local_sem,
    swap_send,
    swap_recv,
    z_send,
    z_recv,
    relay_send,
    x1_send,
    x1_recv,
    x2_send,
    x2_recv,
    own_send,
    own_recv,
    kl_sem,
    plane_send,
    plane_recv,
    dp_send,
    dp_recv,
):
    dp = lax.axis_index("dp")
    head = lax.axis_index("head")
    kv = lax.axis_index("kv")
    row = kv // NX
    col = kv % NX
    right = row * NX + (col + 1) % NX
    left = row * NX + (col + NX - 1) % NX

    def device(d, h, k):
        return (d, h, k)

    def remote(src, dst, send_sem, recv_sem, dev):
        return pltpu.make_async_remote_copy(
            src_ref=src,
            dst_ref=dst,
            send_sem=send_sem,
            recv_sem=recv_sem,
            device_id=dev,
            device_id_type=MESH,
        )

    s_lane = pl.multiple_of(256 + head * 128, 128)
    fill_t = pltpu.make_async_copy(tk_in.at[0], keys.at[kv, :, pl.ds(0, 256)], local_sem.at[0])
    fill_s = pltpu.make_async_copy(sk_in.at[0], keys.at[kv, :, pl.ds(s_lane, 128)], local_sem.at[1])
    fill_q = pltpu.make_async_copy(sq_in.at[0], sq.at[head], local_sem.at[2])
    fill_tq = pltpu.make_async_copy(tq_in.at[0], tq, local_sem.at[3])
    fill_s.start()
    fill_t.start()
    fill_q.start()
    fill_tq.start()

    partner = device(dp, 1 - head, kv)
    near = (
        partner,
        device(dp, head, right),
        device(dp, head, left),
        device(dp, head, (kv + NX) % N_KV),
        device(dp, head, (kv + N_KV - NX) % N_KV),
    )
    barrier = pltpu.get_barrier_semaphore()

    def greet_near(semaphore):
        for peer in near:
            pl.semaphore_signal(semaphore, inc=1, device_id=peer, device_id_type=MESH)

    greet_near(barrier)
    for i in range(1, N_DP):
        pl.semaphore_signal(
            barrier, inc=1, device_id=device((dp + i) % N_DP, head, kv), device_id_type=MESH
        )

    def columns(h):
        return pl.ds(pl.multiple_of(h * DH, DH), DH)

    fill_q.wait()

    def prepare_student(t, _):
        qs[t] = split_scaled(sq[head, :, columns(t)])
        return 0

    lax.fori_loop(0, S_LOCAL, prepare_student, 0)
    bias_col = col * ROWS + lax.broadcasted_iota(jnp.int32, (PIECE, ROWS), 1)
    bias_pos = lax.broadcasted_iota(jnp.int32, (PIECE, ROWS), 0)
    bias_key = bias_pos + (bias_pos // CHUNK) * (ROWS - CHUNK)
    for c in range(2):
        bias[c * PIECE : (c + 1) * PIECE] = jnp.where(bias_key + c * CHUNK <= bias_col, 0.0, NEG)
    fill_s.wait()
    fill_t.wait()
    pl.semaphore_wait(barrier, len(near) + N_DP - 1)

    def own_part(c, side, part, target):
        block = keys.at[kv, pl.ds(c * CHUNK, CHUNK), pl.ds(256 * part, 256)]
        return remote(
            block, block, own_send.at[c, side, part], own_recv.at[c, side, part], device(dp, head, target)
        )

    def start_own(part):
        for c in range(2):
            own_part(c, 0, part, right).start()
            own_part(c, 1, part, left).start()

    swap_s = remote(
        keys.at[kv, :, pl.ds(s_lane, 128)],
        keys.at[kv, :, pl.ds(s_lane, 128)],
        swap_send.at[0],
        swap_recv.at[0],
        partner,
    )
    swap_s.start()
    start_own(0)
    greet_near(levels.at[0])
    swap_q = remote(sq.at[head], sq.at[head], swap_send.at[1], swap_recv.at[1], partner)
    last_row = row == NZ - 1

    @pl.when(last_row)
    def _():
        swap_q.start()


    def student_of(t):
        found = jnp.int32(0)
        for e in range(HT):
            found = jnp.where(table[e % 2, e // 2] == head * T_LOCAL + t, e // 2, found)
        return found

    students = [student_of(t) for t in range(T_LOCAL)]
    for t in range(T_LOCAL):
        student_table[t] = students[t]
        group_table[t] = jnp.where(students[t] >= GROUP, 1, 0)

    def prepare(t, _):
        q = tq[:, columns(t)]
        qy[t] = split_scaled(q)
        s = student_table[t]
        minus_q = jnp.zeros((ROWS, DH), jnp.bfloat16)
        for e in range(S_LOCAL):
            candidate = -sq[head, :, e * DH : (e + 1) * DH]
            minus_q = jnp.where(s == head * S_LOCAL + e, candidate, minus_q)
        qg[t] = jnp.concatenate([q, minus_q], axis=1)
        return 0

    fill_tq.wait()
    lax.fori_loop(0, T_LOCAL, prepare, 0)
    other_lane = pl.multiple_of(384 - head * 128, 128)
    landed_s = remote(
        keys.at[kv, :, pl.ds(other_lane, 128)],
        keys.at[kv, :, pl.ds(other_lane, 128)],
        swap_send.at[0],
        swap_recv.at[0],
        partner,
    )
    landed_s.wait_recv()

    def z_copy(slot_row, c, send_sem, target_row):
        block = keys.at[slot_row * NX + col, pl.ds(c * CHUNK, CHUNK)]
        return remote(
            block, block, send_sem, z_recv.at[slot_row, c], device(dp, head, target_row * NX + col)
        )

    def up(c):
        return z_copy(row, c, z_send.at[0, c], row + 1)

    def down(c):
        return z_copy(row, c, z_send.at[1, c], (row + NZ - 1) % NZ)

    has_up = row < NZ - 1
    has_down = (row == 0, row < 2)

    def forward(slot_row, c):
        return z_copy(slot_row, c, relay_send.at[c], jnp.where(row == 0, NZ - 1, jnp.where(row == NZ - 1, 2, row + 1)))

    def x1(slot_row, c, side, target):
        block = keys.at[slot_row * NX + col, pl.ds(c * CHUNK, CHUNK)]
        return remote(
            block,
            block,
            x1_send.at[slot_row, c, side],
            x1_recv.at[slot_row, c, side],
            device(dp, head, target),
        )

    def x1_arrival(slot_row, c, side, source_col):
        block = keys.at[slot_row * NX + source_col, pl.ds(c * CHUNK, CHUNK)]
        return remote(
            block,
            block,
            x1_send.at[slot_row, c, side],
            x1_recv.at[slot_row, c, side],
            device(dp, head, right),
        )

    def x2(slot_row, c, side, source_col, target):
        block = keys.at[
            slot_row * NX + source_col, pl.ds(c * CHUNK + side * HALF, HALF)
        ]
        return remote(
            block,
            block,
            x2_send.at[slot_row, c, side],
            x2_recv.at[slot_row, c, side],
            device(dp, head, target),
        )

    def own_arrival(c, side, source_col):
        for part in range(2):
            block = keys.at[row * NX + source_col, pl.ds(c * CHUNK, CHUNK), pl.ds(256 * part, 256)]
            remote(
                block,
                block,
                own_send.at[c, side, part],
                own_recv.at[c, side, part],
                device(dp, head, right),
            ).wait_recv()

    left_col = (col + NX - 1) % NX
    right_col = (col + 1) % NX
    far_col = (col + 2) % NX

    def wave(w):
        early = w < 2
        last = row == NZ - 1
        k = w // 2
        r_last = jnp.where(w >= 6, 1, jnp.where(w % 2 == 0, 2, 0))
        c_last = jnp.where(w >= 6, w - 6, (w - 2) // 2)
        r = jnp.where(early, row, jnp.where(last, r_last, row - k))
        c = jnp.where(early, w, jnp.where(last, c_last, w % 2))
        return r, c

    def start_x1(r, c):
        x1(r, c, 0, right).start()
        x1(r, c, 1, left).start()

    def z_event(w):
        r, c = wave(w)
        z_copy(r, c, relay_send.at[c], row).wait_recv()
        start_x1(r, c)

        @pl.when(((row == NZ - 1) & (r == 0)) | ((row == 2) & (r == 1) & (c == 0)))
        def _():
            forward(r, c).start()

    def x_event(w):
        r, c = wave(w)
        x1_arrival(r, c, 0, left_col).wait_recv()
        x2(r, c, 0, left_col, right).start()
        x1_arrival(r, c, 1, right_col).wait_recv()
        x2(r, c, 1, right_col, left).start()

    def d_event(w):
        r, c = wave(w)
        x2(r, c, 0, far_col, right).wait_recv()
        x2(r, c, 1, far_col, right).wait_recv()

    def start_z(c):
        @pl.when(has_up)
        def _():
            up(c).start()

        @pl.when(has_down[c])
        def _():
            down(c).start()

    start_own(1)
    start_z(0)
    start_z(1)

    @pl.when(jnp.logical_not(last_row))
    def _():
        swap_q.start()

    waves = 2 * (row + 1)

    def events(event, *indices):
        for w in indices:

            @pl.when(w < waves)
            def _():
                event(w)

    def next_level(i):
        pl.semaphore_wait(levels.at[i - 1], len(near))
        greet_near(levels.at[i])

    def pieces_of(k):
        return wave(2 * k), wave(2 * k + 1)

    def tile(pieces, lane):
        return jnp.concatenate(
            [
                keys[pl.ds(r * NX, NX), pl.ds(c * CHUNK, CHUNK), pl.ds(lane, 128)].reshape(
                    PIECE, 128
                )
                for r, c in pieces
            ],
            axis=0,
        )

    def product(lhs, rhs):
        return lax.dot_general(lhs, rhs, NT, preferred_element_type=jnp.float32)

    def logits(pieces, t, lane, y_buf):
        k_t = tile(pieces, lane)
        y_buf[...] = product(jnp.concatenate([k_t, k_t], axis=1), qy[t])

    def student_products(pieces, t):
        k_s = tile(pieces, s_lane)
        y_s[...] = product(jnp.concatenate([k_s, k_s], axis=1), qs[t])

    def gaps(pieces, t, lane, g_buf):
        group = group_table[t]
        k_t = tile(pieces, lane)
        k_s = jnp.where(group == 0, tile(pieces, 256), tile(pieces, 384))
        g_buf[...] = product(jnp.concatenate([k_t, k_s], axis=1), qg[t])

    parts_of_tile = [pl.ds(n * SUB, SUB) for n in range(TILE // SUB)]

    def first_weights(y_buf, p_buf):
        def masked(part):
            return (y_buf[part] + bias[part]).reshape(SUB // 8, 8, ROWS)

        m = jnp.max(masked(parts_of_tile[0]), axis=0)
        for part in parts_of_tile[1:]:
            m = jnp.maximum(m, jnp.max(masked(part), axis=0))
        total = jnp.zeros((8, ROWS), jnp.float32)
        for part in parts_of_tile:
            p = jnp.exp2(masked(part) - m[None])
            total = total + jnp.sum(p, axis=0)
            if p_buf is not None:
                p_buf[part] = p.reshape(SUB, ROWS)
        return m, total

    def first_teacher(t, y_buf):
        m, total = first_weights(y_buf, first_p.at[t])
        t_state[t, 0:8] = m
        t_state[t, 8:16] = total

    def first_student(t):
        m, total = first_weights(y_s, None)
        s_state[t, 0:8] = m
        s_state[t, 8:16] = total

    def first_cross(t, g_buf):
        cross = jnp.zeros((8, ROWS), jnp.float32)
        for part in parts_of_tile:
            term = first_p[t, part] * g_buf[part]
            cross = cross + jnp.sum(term.reshape(SUB // 8, 8, ROWS), axis=0)
        t_state[t, 16:24] = cross

    own = pieces_of(0)

    def first_step(j, _):
        logits(own, GROUP + j, 128, y_b)
        student_products(own, j)
        first_teacher(j, y_a)
        logits(own, jnp.minimum(j + 1, GROUP - 1), 0, y_a)
        first_teacher(GROUP + j, y_b)
        first_student(j)
        return 0

    def cross_step(j, _):
        gaps(own, GROUP + j, 128, g_b)
        first_cross(j, g_a)
        gaps(own, j + 1, 0, g_a)
        first_cross(GROUP + j, g_b)
        return 0

    for c in range(2):
        own_arrival(c, 0, left_col)
        x2(row, c, 0, left_col, right).start()
        own_arrival(c, 1, right_col)
        x2(row, c, 1, right_col, left).start()
    next_level(1)
    events(z_event, 2)

    @pl.when(row == 0)
    def _():
        z_copy(1, 1, relay_send.at[1], row).wait_recv()
        forward(1, 1).start()

    events(z_event, 3)
    d_event(0)
    d_event(1)
    logits(own, 0, 0, y_a)
    lax.fori_loop(0, 3, first_step, 0)
    events(x_event, 2)
    lax.fori_loop(3, 5, first_step, 0)
    events(x_event, 3)

    @pl.when(last_row)
    def _():
        events(z_event, 4, 5)

    lax.fori_loop(5, GROUP, first_step, 0)
    remote(sq.at[1 - head], sq.at[1 - head], swap_send.at[1], swap_recv.at[1], partner).wait_recv()
    next_level(2)

    def prepare_far(t, _):
        s = student_table[t]
        minus_q = qg[t, :, DH : 2 * DH]
        for e in range(S_LOCAL):
            candidate = -sq[1 - head, :, e * DH : (e + 1) * DH]
            minus_q = jnp.where(s == (1 - head) * S_LOCAL + e, candidate, minus_q)
        qg[t, :, DH : 2 * DH] = minus_q
        return 0

    lax.fori_loop(0, T_LOCAL, prepare_far, 0)

    def teacher_products(pieces, t, lane, y_buf, g_buf):
        group = group_table[t]
        k_t = tile(pieces, lane)
        k_s = jnp.where(group == 0, tile(pieces, 256), tile(pieces, 384))
        y_buf[...] = product(jnp.concatenate([k_t, k_t], axis=1), qy[t])
        g_buf[...] = product(jnp.concatenate([k_t, k_s], axis=1), qg[t])

    def weights(y_buf, part, running_max):
        y = y_buf[part].reshape(SUB // 8, 8, ROWS)
        new_max = jnp.maximum(running_max, jnp.max(y, axis=0))
        return new_max, jnp.exp2(running_max - new_max), jnp.exp2(y - new_max[None])

    def teacher_update(t, y_buf, g_buf):
        m, total, cross = t_state[t, 0:8], t_state[t, 8:16], t_state[t, 16:24]
        for part in parts_of_tile:
            m, rescale, p = weights(y_buf, part, m)
            total = total * rescale + jnp.sum(p, axis=0)
            cross = cross * rescale + jnp.sum(p * g_buf[part].reshape(p.shape), axis=0)
        t_state[t, 0:8] = m
        t_state[t, 8:16] = total
        t_state[t, 16:24] = cross

    def student_update(t):
        m, total = s_state[t, 0:8], s_state[t, 8:16]
        for part in parts_of_tile:
            m, rescale, p = weights(y_s, part, m)
            total = total * rescale + jnp.sum(p, axis=0)
        s_state[t, 0:8] = m
        s_state[t, 8:16] = total

    def step(now, after, j, _):
        final = j == GROUP - 1
        later = [
            tuple(jnp.where(final, new, old) for old, new in zip(*pair)) for pair in zip(now, after)
        ]
        teacher_products(now, GROUP + j, 128, y_b, g_b)
        student_products(now, j)
        teacher_update(j, y_a, g_a)
        teacher_products(later, jnp.where(final, 0, j + 1), 0, y_a, g_a)
        teacher_update(GROUP + j, y_b, g_b)
        student_update(j)
        return 0

    gaps(own, 0, 0, g_a)
    lax.fori_loop(0, GROUP - 1, cross_step, 0)
    events(d_event, 2, 3)
    gaps(own, T_LOCAL - 1, 128, g_b)
    first_cross(GROUP - 1, g_a)
    teacher_products(pieces_of(jnp.minimum(1, row)), 0, 0, y_a, g_a)
    first_cross(T_LOCAL - 1, g_b)
    next_level(3)

    def stretch(n, _):
        k = n // 3
        part = n % 3

        @pl.when((part == 0) & (k == 1) & jnp.logical_not(last_row))
        def _():
            events(z_event, 4, 5)

        @pl.when(part == jnp.where(last_row & (k == 1), 0, 1))
        def _():
            events(x_event, 2 * k + 2, 2 * k + 3)
            events(z_event, 2 * k + 4, 2 * k + 5)

        @pl.when(part == 2)
        def _():
            events(d_event, 2 * k + 2, 2 * k + 3)

        lax.fori_loop(
            jnp.where(part == 0, 0, jnp.where(part == 1, 2, 6)),
            jnp.where(part == 0, 2, jnp.where(part == 1, 6, GROUP)),
            functools.partial(step, pieces_of(k), pieces_of(jnp.minimum(k + 1, row))),
            0,
        )
        return 0

    lax.fori_loop(3, 3 * (row + 1), stretch, 0)

    lane_row = lax.broadcasted_iota(jnp.int32, (8, ROWS), 0)
    parts = [jnp.zeros((8, ROWS), jnp.float32), jnp.zeros((8, ROWS), jnp.float32)]
    for t in range(T_LOCAL):
        m = t_state[t, 0:8]
        top = jnp.max(m, axis=0, keepdims=True)
        w = jnp.exp2(m - top)
        total = jnp.sum(t_state[t, 8:16] * w, axis=0, keepdims=True)
        cross = jnp.sum(t_state[t, 16:24] * w, axis=0, keepdims=True)
        value = cross / total * SCALE - (top + jnp.log2(total)) * LN2
        for g in range(2):
            parts[g] = parts[g] + jnp.where(lane_row == students[t] - g * GROUP, value, 0.0) * jnp.where(
                (students[t] >= GROUP) == (g == 1), 1.0, 0.0
            )
    home = jnp.zeros((8, ROWS), jnp.float32)
    for t in range(S_LOCAL):
        m = s_state[t, 0:8]
        top = jnp.max(m, axis=0, keepdims=True)
        total = jnp.sum(s_state[t, 8:16] * jnp.exp2(m - top), axis=0, keepdims=True)
        home = home + jnp.where(lane_row == t, (top + jnp.log2(total)) * (2.0 * LN2), 0.0)
    for g in range(2):
        contrib[g] = parts[g] + jnp.where(head == g, home, 0.0)
    pl.semaphore_wait(levels.at[3], len(near))
    kl_copy = remote(contrib.at[1 - head], kl_other, kl_sem.at[0], kl_sem.at[1], partner)
    kl_copy.start()

    me = head * N_KV + kv
    for g in range(2):
        block = jnp.sum(contrib[g], axis=1, keepdims=True)
        sums_plane[2 * N_KV + g] = jnp.broadcast_to(block, (8, 128))

    def plane_copy(i):
        peer = (me + i) % (2 * N_KV)
        return remote(
            sums_plane.at[2 * N_KV + peer // N_KV],
            sums_plane.at[me],
            plane_send.at[i],
            plane_recv.at[me],
            device(dp, peer // N_KV, peer % N_KV),
        )

    def plane_start(i, _):
        plane_copy(i).start()
        return 0

    lax.fori_loop(1, 2 * N_KV, plane_start, 0)

    swap_s.wait_send()
    swap_q.wait_send()
    for c in range(2):

        @pl.when(has_up)
        def _():
            up(c).wait_send()

        @pl.when(has_down[c])
        def _():
            down(c).wait_send()

        @pl.when(row == NZ - 1)
        def _():
            forward(0, c).wait_send()

    @pl.when(row == 0)
    def _():
        forward(1, 1).wait_send()

    @pl.when(row == 2)
    def _():
        forward(1, 0).wait_send()

    for c in range(2):
        for part in range(2):
            own_part(c, 0, part, right).wait_send()
            own_part(c, 1, part, left).wait_send()

    def drain(w, _):
        r, c = wave(w)

        @pl.when(w > 1)
        def _():
            x1(r, c, 0, right).wait_send()
            x1(r, c, 1, left).wait_send()

        x2(r, c, 0, left_col, right).wait_send()
        x2(r, c, 1, right_col, left).wait_send()
        return 0

    lax.fori_loop(0, waves, drain, 0)

    kl_copy.wait()
    kl_rows = contrib[head] + kl_other[...]
    for t in range(S_LOCAL):
        kl_out[t] = kl_rows[t : t + 1]

    def plane_wait(i, total):
        source = (me + i) % (2 * N_KV)
        remote(
            sums_plane.at[source],
            sums_plane.at[source],
            plane_send.at[i],
            plane_recv.at[source],
            partner,
        ).wait_recv()
        return total + sums_plane[source]

    plane_total = lax.fori_loop(1, 2 * N_KV, plane_wait, sums_plane[2 * N_KV + head])
    sums_dp[N_DP] = plane_total

    def dp_copy(i):
        return remote(
            sums_dp.at[N_DP],
            sums_dp.at[dp],
            dp_send.at[i],
            dp_recv.at[dp],
            device((dp + i) % N_DP, head, kv),
        )

    for i in range(1, N_DP):
        dp_copy(i).start()
    def plane_drain(i, _):
        plane_copy(i).wait_send()
        return 0

    lax.fori_loop(1, 2 * N_KV, plane_drain, 0)
    grand = plane_total
    for i in range(1, N_DP):
        source = (dp + i) % N_DP
        remote(
            sums_dp.at[source], sums_dp.at[source], dp_send.at[i], dp_recv.at[source], partner
        ).wait_recv()
        grand = grand + sums_dp[source]
    diagonal = lax.broadcasted_iota(jnp.int32, (8, 128), 0) == lax.broadcasted_iota(
        jnp.int32, (8, 128), 1
    )
    loss_out[...] = jnp.sum(jnp.where(diagonal, grand, 0.0), axis=0, keepdims=True) * (
        1.0 / (N_DP * N_KV * ROWS)
    )

    for i in range(1, N_DP):
        dp_copy(i).wait_send()


def per_device(teacher_query, teacher_key, student_query, student_key, pair_table):
    vmem = pl.BlockSpec(memory_space=pltpu.VMEM)
    anywhere = pl.BlockSpec(memory_space=pl.ANY)
    dma = pltpu.SemaphoreType.DMA
    f32, bf16 = jnp.float32, jnp.bfloat16
    kl, loss = pl.pallas_call(
        kernel,
        out_shape=(
            jax.ShapeDtypeStruct((S_LOCAL, 1, ROWS), f32),
            jax.ShapeDtypeStruct((1, 128), f32),
        ),
        in_specs=[pl.BlockSpec(memory_space=pltpu.SMEM), anywhere, anywhere, anywhere, anywhere],
        out_specs=(vmem, vmem),
        scratch_shapes=[
            pltpu.VMEM((N_KV, ROWS, 512), bf16),
            pltpu.VMEM((ROWS, T_LOCAL * DH), bf16),
            pltpu.VMEM((2, ROWS, S_LOCAL * DH), bf16),
            pltpu.VMEM((T_LOCAL, ROWS, 256), bf16),
            pltpu.VMEM((T_LOCAL, ROWS, 256), bf16),
            pltpu.VMEM((S_LOCAL, ROWS, 256), bf16),
            pltpu.VMEM((T_LOCAL, 24, ROWS), f32),
            pltpu.VMEM((S_LOCAL, 16, ROWS), f32),
            pltpu.VMEM((TILE, ROWS), f32),
            pltpu.VMEM((TILE, ROWS), f32),
            pltpu.VMEM((TILE, ROWS), f32),
            pltpu.VMEM((TILE, ROWS), f32),
            pltpu.VMEM((TILE, ROWS), f32),
            pltpu.VMEM((T_LOCAL, TILE, ROWS), f32),
            pltpu.VMEM((TILE, ROWS), f32),
            pltpu.VMEM((2, 8, ROWS), f32),
            pltpu.VMEM((8, ROWS), f32),
            pltpu.VMEM((2 * N_KV + 2, 8, 128), f32),
            pltpu.VMEM((N_DP + 1, 8, 128), f32),
            pltpu.SMEM((T_LOCAL,), jnp.int32),
            pltpu.SMEM((T_LOCAL,), jnp.int32),
            pltpu.SemaphoreType.REGULAR((4,)),
            dma((4,)),
            dma((2,)),
            dma((2,)),
            dma((2, 2)),
            dma((NZ, 2)),
            dma((2,)),
            dma((NZ, 2, 2)),
            dma((NZ, 2, 2)),
            dma((NZ, 2, 2)),
            dma((NZ, 2, 2)),
            dma((2, 2, 2)),
            dma((2, 2, 2)),
            dma((2,)),
            dma((2 * N_KV,)),
            dma((2 * N_KV,)),
            dma((N_DP,)),
            dma((N_DP,)),
        ],
        compiler_params=pltpu.CompilerParams(
            collective_id=0, has_side_effects=True, vmem_limit_bytes=60 * 1024 * 1024
        ),
    )(pair_table.T, teacher_query, teacher_key, student_query, student_key)
    return jnp.transpose(kl, (1, 0, 2)), loss[0, :S_LOCAL]


def solution(mesh):
    spec = P("dp", "kv", "head")
    return jax.shard_map(
        per_device,
        mesh=mesh,
        in_specs=(spec, spec, spec, spec, P()),
        out_specs=(P("dp", "head", "kv"), P("head")),
        check_vma=False,
    )
```

```python
import functools
import math

import jax
import jax.numpy as jnp
from jax import lax
from jax.experimental import pallas as pl
from jax.experimental.pallas import tpu as pltpu
from jax.sharding import PartitionSpec as P

HT = 28
HS = 14
DH = 128
GROUP = 7
NX = 4
NZ = 4
N_KV = NX * NZ
N_DP = 8
ROWS = 256
CHUNK = 128
HALF = CHUNK // 2
PIECE = NX * CHUNK
TILE = 2 * PIECE
SUB = 128
T_LOCAL = 14
S_LOCAL = 7
SCALE = 1.0 / math.sqrt(DH)
LOG2E = math.log2(math.e)
LN2 = math.log(2.0)
NEG = -1e30
MESH = pl.DeviceIdType.MESH
NT = (((1,), (1,)), ((), ()))


def split_scaled(q):
    scaled = q.astype(jnp.float32) * (SCALE * LOG2E)
    hi = scaled.astype(jnp.bfloat16)
    lo = (scaled - hi.astype(jnp.float32)).astype(jnp.bfloat16)
    return jnp.concatenate([hi, lo], axis=1)


def kernel(
    table,
    tq_in,
    tk_in,
    sq_in,
    sk_in,
    kl_out,
    loss_out,
    keys,
    tq,
    sq,
    qy,
    qg,
    qs,
    t_state,
    s_state,
    y_a,
    g_a,
    y_b,
    g_b,
    y_s,
    first_p,
    bias,
    contrib,
    kl_other,
    sums_plane,
    sums_dp,
    group_table,
    student_table,
    levels,
    local_sem,
    swap_send,
    swap_recv,
    z_send,
    z_recv,
    relay_send,
    x1_send,
    x1_recv,
    x2_send,
    x2_recv,
    own_send,
    own_recv,
    kl_sem,
    plane_send,
    plane_recv,
    dp_send,
    dp_recv,
):
    dp = lax.axis_index("dp")
    head = lax.axis_index("head")
    kv = lax.axis_index("kv")
    row = kv // NX
    col = kv % NX
    right = row * NX + (col + 1) % NX
    left = row * NX + (col + NX - 1) % NX

    def device(d, h, k):
        return (d, h, k)

    def remote(src, dst, send_sem, recv_sem, dev):
        return pltpu.make_async_remote_copy(
            src_ref=src,
            dst_ref=dst,
            send_sem=send_sem,
            recv_sem=recv_sem,
            device_id=dev,
            device_id_type=MESH,
        )

    s_lane = pl.multiple_of(256 + head * 128, 128)
    fill_t = pltpu.make_async_copy(tk_in.at[0], keys.at[kv, :, pl.ds(0, 256)], local_sem.at[0])
    fill_s = pltpu.make_async_copy(sk_in.at[0], keys.at[kv, :, pl.ds(s_lane, 128)], local_sem.at[1])
    fill_q = pltpu.make_async_copy(sq_in.at[0], sq.at[head], local_sem.at[2])
    fill_tq = pltpu.make_async_copy(tq_in.at[0], tq, local_sem.at[3])
    fill_s.start()
    fill_t.start()
    fill_q.start()
    fill_tq.start()

    partner = device(dp, 1 - head, kv)
    near = (
        partner,
        device(dp, head, right),
        device(dp, head, left),
        device(dp, head, (kv + NX) % N_KV),
        device(dp, head, (kv + N_KV - NX) % N_KV),
    )
    barrier = pltpu.get_barrier_semaphore()

    def greet_near(semaphore):
        for peer in near:
            pl.semaphore_signal(semaphore, inc=1, device_id=peer, device_id_type=MESH)

    greet_near(barrier)
    for i in range(1, N_DP):
        pl.semaphore_signal(
            barrier, inc=1, device_id=device((dp + i) % N_DP, head, kv), device_id_type=MESH
        )

    def columns(h):
        return pl.ds(pl.multiple_of(h * DH, DH), DH)

    fill_q.wait()

    def prepare_student(t, _):
        qs[t] = split_scaled(sq[head, :, columns(t)])
        return 0

    lax.fori_loop(0, S_LOCAL, prepare_student, 0)
    bias_col = col * ROWS + lax.broadcasted_iota(jnp.int32, (PIECE, ROWS), 1)
    bias_pos = lax.broadcasted_iota(jnp.int32, (PIECE, ROWS), 0)
    bias_key = bias_pos + (bias_pos // CHUNK) * (ROWS - CHUNK)
    for c in range(2):
        bias[c * PIECE : (c + 1) * PIECE] = jnp.where(bias_key + c * CHUNK <= bias_col, 0.0, NEG)
    fill_s.wait()
    fill_t.wait()
    pl.semaphore_wait(barrier, len(near) + N_DP - 1)

    def own_part(c, side, part, target):
        block = keys.at[kv, pl.ds(c * CHUNK, CHUNK), pl.ds(256 * part, 256)]
        return remote(
            block, block, own_send.at[c, side, part], own_recv.at[c, side, part], device(dp, head, target)
        )

    def start_own(part):
        for c in range(2):
            own_part(c, 0, part, right).start()
            own_part(c, 1, part, left).start()

    swap_s = remote(
        keys.at[kv, :, pl.ds(s_lane, 128)],
        keys.at[kv, :, pl.ds(s_lane, 128)],
        swap_send.at[0],
        swap_recv.at[0],
        partner,
    )
    swap_s.start()
    start_own(0)
    greet_near(levels.at[0])
    swap_q = remote(sq.at[head], sq.at[head], swap_send.at[1], swap_recv.at[1], partner)
    last_row = row == NZ - 1

    @pl.when(last_row)
    def _():
        swap_q.start()


    def student_of(t):
        found = jnp.int32(0)
        for e in range(HT):
            found = jnp.where(table[e % 2, e // 2] == head * T_LOCAL + t, e // 2, found)
        return found

    students = [student_of(t) for t in range(T_LOCAL)]
    for t in range(T_LOCAL):
        student_table[t] = students[t]
        group_table[t] = jnp.where(students[t] >= GROUP, 1, 0)

    def prepare(t, _):
        q = tq[:, columns(t)]
        qy[t] = split_scaled(q)
        s = student_table[t]
        minus_q = jnp.zeros((ROWS, DH), jnp.bfloat16)
        for e in range(S_LOCAL):
            candidate = -sq[head, :, e * DH : (e + 1) * DH]
            minus_q = jnp.where(s == head * S_LOCAL + e, candidate, minus_q)
        qg[t] = jnp.concatenate([q, minus_q], axis=1)
        return 0

    fill_tq.wait()
    lax.fori_loop(0, T_LOCAL, prepare, 0)
    other_lane = pl.multiple_of(384 - head * 128, 128)
    landed_s = remote(
        keys.at[kv, :, pl.ds(other_lane, 128)],
        keys.at[kv, :, pl.ds(other_lane, 128)],
        swap_send.at[0],
        swap_recv.at[0],
        partner,
    )
    landed_s.wait_recv()

    def z_copy(slot_row, c, send_sem, target_row):
        block = keys.at[slot_row * NX + col, pl.ds(c * CHUNK, CHUNK)]
        return remote(
            block, block, send_sem, z_recv.at[slot_row, c], device(dp, head, target_row * NX + col)
        )

    def up(c):
        return z_copy(row, c, z_send.at[0, c], row + 1)

    def down(c):
        return z_copy(row, c, z_send.at[1, c], (row + NZ - 1) % NZ)

    has_up = row < NZ - 1
    has_down = (row == 0, row < 2)

    def forward(slot_row, c):
        return z_copy(slot_row, c, relay_send.at[c], jnp.where(row == 0, NZ - 1, jnp.where(row == NZ - 1, 2, row + 1)))

    def x1(slot_row, c, side, target):
        block = keys.at[slot_row * NX + col, pl.ds(c * CHUNK, CHUNK)]
        return remote(
            block,
            block,
            x1_send.at[slot_row, c, side],
            x1_recv.at[slot_row, c, side],
            device(dp, head, target),
        )

    def x1_arrival(slot_row, c, side, source_col):
        block = keys.at[slot_row * NX + source_col, pl.ds(c * CHUNK, CHUNK)]
        return remote(
            block,
            block,
            x1_send.at[slot_row, c, side],
            x1_recv.at[slot_row, c, side],
            device(dp, head, right),
        )

    def x2(slot_row, c, side, source_col, target):
        block = keys.at[
            slot_row * NX + source_col, pl.ds(c * CHUNK + side * HALF, HALF)
        ]
        return remote(
            block,
            block,
            x2_send.at[slot_row, c, side],
            x2_recv.at[slot_row, c, side],
            device(dp, head, target),
        )

    def own_arrival(c, side, source_col):
        for part in range(2):
            block = keys.at[row * NX + source_col, pl.ds(c * CHUNK, CHUNK), pl.ds(256 * part, 256)]
            remote(
                block,
                block,
                own_send.at[c, side, part],
                own_recv.at[c, side, part],
                device(dp, head, right),
            ).wait_recv()

    left_col = (col + NX - 1) % NX
    right_col = (col + 1) % NX
    far_col = (col + 2) % NX

    def wave(w):
        early = w < 2
        last = row == NZ - 1
        k = w // 2
        r_last = jnp.where(w >= 6, 1, jnp.where(w % 2 == 0, 2, 0))
        c_last = jnp.where(w >= 6, w - 6, (w - 2) // 2)
        r = jnp.where(early, row, jnp.where(last, r_last, row - k))
        c = jnp.where(early, w, jnp.where(last, c_last, w % 2))
        return r, c

    def start_x1(r, c):
        x1(r, c, 0, right).start()
        x1(r, c, 1, left).start()

    def z_event(w):
        r, c = wave(w)
        z_copy(r, c, relay_send.at[c], row).wait_recv()
        start_x1(r, c)

        @pl.when(((row == NZ - 1) & (r == 0)) | ((row == 2) & (r == 1) & (c == 0)))
        def _():
            forward(r, c).start()

    def x_event(w):
        r, c = wave(w)
        x1_arrival(r, c, 0, left_col).wait_recv()
        x2(r, c, 0, left_col, right).start()
        x1_arrival(r, c, 1, right_col).wait_recv()
        x2(r, c, 1, right_col, left).start()

    def d_event(w):
        r, c = wave(w)
        x2(r, c, 0, far_col, right).wait_recv()
        x2(r, c, 1, far_col, right).wait_recv()

    def start_z(c):
        @pl.when(has_up)
        def _():
            up(c).start()

        @pl.when(has_down[c])
        def _():
            down(c).start()

    start_own(1)
    start_z(0)
    start_z(1)

    @pl.when(jnp.logical_not(last_row))
    def _():
        swap_q.start()

    waves = 2 * (row + 1)

    def events(event, *indices):
        for w in indices:

            @pl.when(w < waves)
            def _():
                event(w)

    def next_level(i):
        pl.semaphore_wait(levels.at[i - 1], len(near))
        greet_near(levels.at[i])

    def pieces_of(k):
        return wave(2 * k), wave(2 * k + 1)

    def tile(pieces, lane):
        return jnp.concatenate(
            [
                keys[pl.ds(r * NX, NX), pl.ds(c * CHUNK, CHUNK), pl.ds(lane, 128)].reshape(
                    PIECE, 128
                )
                for r, c in pieces
            ],
            axis=0,
        )

    def product(lhs, rhs):
        return lax.dot_general(lhs, rhs, NT, preferred_element_type=jnp.float32)

    def logits(pieces, t, lane, y_buf):
        k_t = tile(pieces, lane)
        y_buf[...] = product(jnp.concatenate([k_t, k_t], axis=1), qy[t])

    def student_products(pieces, t):
        k_s = tile(pieces, s_lane)
        y_s[...] = product(jnp.concatenate([k_s, k_s], axis=1), qs[t])

    def gaps(pieces, t, lane, g_buf):
        group = group_table[t]
        k_t = tile(pieces, lane)
        k_s = jnp.where(group == 0, tile(pieces, 256), tile(pieces, 384))
        g_buf[...] = product(jnp.concatenate([k_t, k_s], axis=1), qg[t])

    parts_of_tile = [pl.ds(n * SUB, SUB) for n in range(TILE // SUB)]

    def first_weights(y_buf, p_buf):
        def masked(part):
            return (y_buf[part] + bias[part]).reshape(SUB // 8, 8, ROWS)

        m = jnp.max(masked(parts_of_tile[0]), axis=0)
        for part in parts_of_tile[1:]:
            m = jnp.maximum(m, jnp.max(masked(part), axis=0))
        total = jnp.zeros((8, ROWS), jnp.float32)
        for part in parts_of_tile:
            p = jnp.exp2(masked(part) - m[None])
            total = total + jnp.sum(p, axis=0)
            if p_buf is not None:
                p_buf[part] = p.reshape(SUB, ROWS)
        return m, total

    def first_teacher(t, y_buf):
        m, total = first_weights(y_buf, first_p.at[t])
        t_state[t, 0:8] = m
        t_state[t, 8:16] = total

    def first_student(t):
        m, total = first_weights(y_s, None)
        s_state[t, 0:8] = m
        s_state[t, 8:16] = total

    def first_cross(t, g_buf):
        cross = jnp.zeros((8, ROWS), jnp.float32)
        for part in parts_of_tile:
            term = first_p[t, part] * g_buf[part]
            cross = cross + jnp.sum(term.reshape(SUB // 8, 8, ROWS), axis=0)
        t_state[t, 16:24] = cross

    own = pieces_of(0)

    def first_step(j, _):
        logits(own, GROUP + j, 128, y_b)
        student_products(own, j)
        first_teacher(j, y_a)
        logits(own, jnp.minimum(j + 1, GROUP - 1), 0, y_a)
        first_teacher(GROUP + j, y_b)
        first_student(j)
        return 0

    def cross_step(j, _):
        gaps(own, GROUP + j, 128, g_b)
        first_cross(j, g_a)
        gaps(own, j + 1, 0, g_a)
        first_cross(GROUP + j, g_b)
        return 0

    for c in range(2):
        own_arrival(c, 0, left_col)
        x2(row, c, 0, left_col, right).start()
        own_arrival(c, 1, right_col)
        x2(row, c, 1, right_col, left).start()
    next_level(1)
    events(z_event, 2)

    @pl.when(row == 0)
    def _():
        z_copy(1, 1, relay_send.at[1], row).wait_recv()
        forward(1, 1).start()

    events(z_event, 3)
    d_event(0)
    d_event(1)
    logits(own, 0, 0, y_a)
    lax.fori_loop(0, 3, first_step, 0)
    events(x_event, 2)
    lax.fori_loop(3, 5, first_step, 0)
    events(x_event, 3)

    @pl.when(last_row)
    def _():
        events(z_event, 4, 5)

    lax.fori_loop(5, GROUP, first_step, 0)
    remote(sq.at[1 - head], sq.at[1 - head], swap_send.at[1], swap_recv.at[1], partner).wait_recv()
    next_level(2)

    def prepare_far(t, _):
        s = student_table[t]
        minus_q = qg[t, :, DH : 2 * DH]
        for e in range(S_LOCAL):
            candidate = -sq[1 - head, :, e * DH : (e + 1) * DH]
            minus_q = jnp.where(s == (1 - head) * S_LOCAL + e, candidate, minus_q)
        qg[t, :, DH : 2 * DH] = minus_q
        return 0

    lax.fori_loop(0, T_LOCAL, prepare_far, 0)

    def teacher_products(pieces, t, lane, y_buf, g_buf):
        group = group_table[t]
        k_t = tile(pieces, lane)
        k_s = jnp.where(group == 0, tile(pieces, 256), tile(pieces, 384))
        y_buf[...] = product(jnp.concatenate([k_t, k_t], axis=1), qy[t])
        g_buf[...] = product(jnp.concatenate([k_t, k_s], axis=1), qg[t])

    def weights(y_buf, part, running_max):
        y = y_buf[part].reshape(SUB // 8, 8, ROWS)
        new_max = jnp.maximum(running_max, jnp.max(y, axis=0))
        return new_max, jnp.exp2(running_max - new_max), jnp.exp2(y - new_max[None])

    def teacher_update(t, y_buf, g_buf):
        m, total, cross = t_state[t, 0:8], t_state[t, 8:16], t_state[t, 16:24]
        for part in parts_of_tile:
            m, rescale, p = weights(y_buf, part, m)
            total = total * rescale + jnp.sum(p, axis=0)
            cross = cross * rescale + jnp.sum(p * g_buf[part].reshape(p.shape), axis=0)
        t_state[t, 0:8] = m
        t_state[t, 8:16] = total
        t_state[t, 16:24] = cross

    def student_update(t):
        m, total = s_state[t, 0:8], s_state[t, 8:16]
        for part in parts_of_tile:
            m, rescale, p = weights(y_s, part, m)
            total = total * rescale + jnp.sum(p, axis=0)
        s_state[t, 0:8] = m
        s_state[t, 8:16] = total

    def step(now, after, j, _):
        final = j == GROUP - 1
        later = [
            tuple(jnp.where(final, new, old) for old, new in zip(*pair)) for pair in zip(now, after)
        ]
        teacher_products(now, GROUP + j, 128, y_b, g_b)
        teacher_update(j, y_a, g_a)
        student_products(now, j)
        teacher_update(GROUP + j, y_b, g_b)
        teacher_products(later, jnp.where(final, 0, j + 1), 0, y_a, g_a)
        student_update(j)
        return 0

    gaps(own, 0, 0, g_a)
    lax.fori_loop(0, GROUP - 1, cross_step, 0)
    events(d_event, 2, 3)
    gaps(own, T_LOCAL - 1, 128, g_b)
    first_cross(GROUP - 1, g_a)
    teacher_products(pieces_of(jnp.minimum(1, row)), 0, 0, y_a, g_a)
    first_cross(T_LOCAL - 1, g_b)
    next_level(3)

    def stretch(n, _):
        k = n // 3
        part = n % 3

        @pl.when((part == 0) & (k == 1) & jnp.logical_not(last_row))
        def _():
            events(z_event, 4, 5)

        @pl.when(part == jnp.where(last_row & (k == 1), 0, 1))
        def _():
            events(x_event, 2 * k + 2, 2 * k + 3)
            events(z_event, 2 * k + 4, 2 * k + 5)

        @pl.when(part == 2)
        def _():
            events(d_event, 2 * k + 2, 2 * k + 3)

        lax.fori_loop(
            jnp.where(part == 0, 0, jnp.where(part == 1, 2, 6)),
            jnp.where(part == 0, 2, jnp.where(part == 1, 6, GROUP)),
            functools.partial(step, pieces_of(k), pieces_of(jnp.minimum(k + 1, row))),
            0,
        )
        return 0

    lax.fori_loop(3, 3 * (row + 1), stretch, 0)

    lane_row = lax.broadcasted_iota(jnp.int32, (8, ROWS), 0)
    parts = [jnp.zeros((8, ROWS), jnp.float32), jnp.zeros((8, ROWS), jnp.float32)]
    for t in range(T_LOCAL):
        m = t_state[t, 0:8]
        top = jnp.max(m, axis=0, keepdims=True)
        w = jnp.exp2(m - top)
        total = jnp.sum(t_state[t, 8:16] * w, axis=0, keepdims=True)
        cross = jnp.sum(t_state[t, 16:24] * w, axis=0, keepdims=True)
        value = cross / total * SCALE - (top + jnp.log2(total)) * LN2
        for g in range(2):
            parts[g] = parts[g] + jnp.where(lane_row == students[t] - g * GROUP, value, 0.0) * jnp.where(
                (students[t] >= GROUP) == (g == 1), 1.0, 0.0
            )
    home = jnp.zeros((8, ROWS), jnp.float32)
    for t in range(S_LOCAL):
        m = s_state[t, 0:8]
        top = jnp.max(m, axis=0, keepdims=True)
        total = jnp.sum(s_state[t, 8:16] * jnp.exp2(m - top), axis=0, keepdims=True)
        home = home + jnp.where(lane_row == t, (top + jnp.log2(total)) * (2.0 * LN2), 0.0)
    for g in range(2):
        contrib[g] = parts[g] + jnp.where(head == g, home, 0.0)
    pl.semaphore_wait(levels.at[3], len(near))
    kl_copy = remote(contrib.at[1 - head], kl_other, kl_sem.at[0], kl_sem.at[1], partner)
    kl_copy.start()

    me = head * N_KV + kv
    for g in range(2):
        block = jnp.sum(contrib[g], axis=1, keepdims=True)
        sums_plane[2 * N_KV + g] = jnp.broadcast_to(block, (8, 128))

    def plane_copy(i):
        peer = (me + i) % (2 * N_KV)
        return remote(
            sums_plane.at[2 * N_KV + peer // N_KV],
            sums_plane.at[me],
            plane_send.at[i],
            plane_recv.at[me],
            device(dp, peer // N_KV, peer % N_KV),
        )

    def plane_start(i, _):
        plane_copy(i).start()
        return 0

    lax.fori_loop(1, 2 * N_KV, plane_start, 0)

    swap_s.wait_send()
    swap_q.wait_send()
    for c in range(2):

        @pl.when(has_up)
        def _():
            up(c).wait_send()

        @pl.when(has_down[c])
        def _():
            down(c).wait_send()

        @pl.when(row == NZ - 1)
        def _():
            forward(0, c).wait_send()

    @pl.when(row == 0)
    def _():
        forward(1, 1).wait_send()

    @pl.when(row == 2)
    def _():
        forward(1, 0).wait_send()

    for c in range(2):
        for part in range(2):
            own_part(c, 0, part, right).wait_send()
            own_part(c, 1, part, left).wait_send()

    def drain(w, _):
        r, c = wave(w)

        @pl.when(w > 1)
        def _():
            x1(r, c, 0, right).wait_send()
            x1(r, c, 1, left).wait_send()

        x2(r, c, 0, left_col, right).wait_send()
        x2(r, c, 1, right_col, left).wait_send()
        return 0

    lax.fori_loop(0, waves, drain, 0)

    kl_copy.wait()
    kl_rows = contrib[head] + kl_other[...]
    for t in range(S_LOCAL):
        kl_out[t] = kl_rows[t : t + 1]

    def plane_wait(i, total):
        source = (me + i) % (2 * N_KV)
        remote(
            sums_plane.at[source],
            sums_plane.at[source],
            plane_send.at[i],
            plane_recv.at[source],
            partner,
        ).wait_recv()
        return total + sums_plane[source]

    plane_total = lax.fori_loop(1, 2 * N_KV, plane_wait, sums_plane[2 * N_KV + head])
    sums_dp[N_DP] = plane_total

    def dp_copy(i):
        return remote(
            sums_dp.at[N_DP],
            sums_dp.at[dp],
            dp_send.at[i],
            dp_recv.at[dp],
            device((dp + i) % N_DP, head, kv),
        )

    for i in range(1, N_DP):
        dp_copy(i).start()
    def plane_drain(i, _):
        plane_copy(i).wait_send()
        return 0

    lax.fori_loop(1, 2 * N_KV, plane_drain, 0)
    grand = plane_total
    for i in range(1, N_DP):
        source = (dp + i) % N_DP
        remote(
            sums_dp.at[source], sums_dp.at[source], dp_send.at[i], dp_recv.at[source], partner
        ).wait_recv()
        grand = grand + sums_dp[source]
    diagonal = lax.broadcasted_iota(jnp.int32, (8, 128), 0) == lax.broadcasted_iota(
        jnp.int32, (8, 128), 1
    )
    loss_out[...] = jnp.sum(jnp.where(diagonal, grand, 0.0), axis=0, keepdims=True) * (
        1.0 / (N_DP * N_KV * ROWS)
    )

    for i in range(1, N_DP):
        dp_copy(i).wait_send()


def per_device(teacher_query, teacher_key, student_query, student_key, pair_table):
    vmem = pl.BlockSpec(memory_space=pltpu.VMEM)
    anywhere = pl.BlockSpec(memory_space=pl.ANY)
    dma = pltpu.SemaphoreType.DMA
    f32, bf16 = jnp.float32, jnp.bfloat16
    kl, loss = pl.pallas_call(
        kernel,
        out_shape=(
            jax.ShapeDtypeStruct((S_LOCAL, 1, ROWS), f32),
            jax.ShapeDtypeStruct((1, 128), f32),
        ),
        in_specs=[pl.BlockSpec(memory_space=pltpu.SMEM), anywhere, anywhere, anywhere, anywhere],
        out_specs=(vmem, vmem),
        scratch_shapes=[
            pltpu.VMEM((N_KV, ROWS, 512), bf16),
            pltpu.VMEM((ROWS, T_LOCAL * DH), bf16),
            pltpu.VMEM((2, ROWS, S_LOCAL * DH), bf16),
            pltpu.VMEM((T_LOCAL, ROWS, 256), bf16),
            pltpu.VMEM((T_LOCAL, ROWS, 256), bf16),
            pltpu.VMEM((S_LOCAL, ROWS, 256), bf16),
            pltpu.VMEM((T_LOCAL, 24, ROWS), f32),
            pltpu.VMEM((S_LOCAL, 16, ROWS), f32),
            pltpu.VMEM((TILE, ROWS), f32),
            pltpu.VMEM((TILE, ROWS), f32),
            pltpu.VMEM((TILE, ROWS), f32),
            pltpu.VMEM((TILE, ROWS), f32),
            pltpu.VMEM((TILE, ROWS), f32),
            pltpu.VMEM((T_LOCAL, TILE, ROWS), f32),
            pltpu.VMEM((TILE, ROWS), f32),
            pltpu.VMEM((2, 8, ROWS), f32),
            pltpu.VMEM((8, ROWS), f32),
            pltpu.VMEM((2 * N_KV + 2, 8, 128), f32),
            pltpu.VMEM((N_DP + 1, 8, 128), f32),
            pltpu.SMEM((T_LOCAL,), jnp.int32),
            pltpu.SMEM((T_LOCAL,), jnp.int32),
            pltpu.SemaphoreType.REGULAR((4,)),
            dma((4,)),
            dma((2,)),
            dma((2,)),
            dma((2, 2)),
            dma((NZ, 2)),
            dma((2,)),
            dma((NZ, 2, 2)),
            dma((NZ, 2, 2)),
            dma((NZ, 2, 2)),
            dma((NZ, 2, 2)),
            dma((2, 2, 2)),
            dma((2, 2, 2)),
            dma((2,)),
            dma((2 * N_KV,)),
            dma((2 * N_KV,)),
            dma((N_DP,)),
            dma((N_DP,)),
        ],
        compiler_params=pltpu.CompilerParams(
            collective_id=0, has_side_effects=True, vmem_limit_bytes=60 * 1024 * 1024
        ),
    )(pair_table.T, teacher_query, teacher_key, student_query, student_key)
    return jnp.transpose(kl, (1, 0, 2)), loss[0, :S_LOCAL]


def solution(mesh):
    spec = P("dp", "kv", "head")
    return jax.shard_map(
        per_device,
        mesh=mesh,
        in_specs=(spec, spec, spec, spec, P()),
        out_specs=(P("dp", "head", "kv"), P("head")),
        check_vma=False,
    )
```
